32 devices in a mesh: dp: 8 (over z, y), tensor: 4 (over x, core).
Axes of the slice: x: 2, y: 2, z: 4, core: 2. Of those that a mesh axis runs over, the one named last changes fastest.
Arguments:
- hidden: bfloat16 [8, 1024, 1024], P('dp', 'tensor'), may hold values from -6 to 6
- encoder: bfloat16 [8, 1024, 1024], P('dp', 'tensor'), may hold values from -6 to 6
- prefix: int32 [8], P('dp'), may hold values from 102 to 512
- query_self: bfloat16 [1, 1024, 1024], P(None, 'dp', 'tensor'), may hold values from -0.1875 to 0.1875
- key_self: bfloat16 [1, 1024, 1024], P(None, 'dp', 'tensor'), may hold values from -0.1875 to 0.1875
- value_self: bfloat16 [1, 1024, 1024], P(None, 'dp', 'tensor'), may hold values from -0.1875 to 0.1875
- output_self: bfloat16 [1, 1024, 1024], P(None, 'tensor', 'dp'), may hold values from -3 to 3
- cross_query_matrix: bfloat16 [1, 1024, 1024], P(None, 'dp', 'tensor'), may hold values from -0.1875 to 0.1875
- key_cross: bfloat16 [1, 1024, 1024], P(None, 'dp', 'tensor'), may hold values from -0.1875 to 0.1875
- value_cross: bfloat16 [1, 1024, 1024], P(None, 'dp', 'tensor'), may hold values from -0.1875 to 0.1875
- output_cross: bfloat16 [1, 1024, 1024], P(None, 'tensor', 'dp'), may hold values from -3 to 3
- expand: bfloat16 [1, 1024, 4096], P(None, 'dp', 'tensor'), may hold values from -0.1875 to 0.1875
- shrink: bfloat16 [1, 4096, 1024], P(None, 'tensor', 'dp'), may hold values from -0.09375 to 0.09375
- norm_gains: float32 [1, 3, 1024], replicated, may hold values from 0.25 to 1.75
- biases: float32 [1, 9, 1024], replicated, may hold values from -1.8 to 1.8
- self_out_bias: float32 [1, 1024], replicated, may hold values from -1.8 to 1.8
- expand_bias: float32 [1, 4096], replicated, may hold values from -1.8 to 1.8
- cotangent: bfloat16 [8, 1024, 1024], P('dp', 'tensor'), may hold values from -6 to 6
Outputs:
- block_output: bfloat16 [8, 1024, 1024], P('dp', 'tensor')
- grad_hidden: float32 [8, 1024, 1024], P('dp', 'tensor')
- grad_encoder: float32 [8, 1024, 1024], P('dp', 'tensor')
- grad_query_self: float32 [1, 1024, 1024], P(None, 'dp', 'tensor')
- grad_key_self: float32 [1, 1024, 1024], P(None, 'dp', 'tensor')
- grad_value_self: float32 [1, 1024, 1024], P(None, 'dp', 'tensor')
- grad_output_self: float32 [1, 1024, 1024], P(None, 'tensor', 'dp')
- grad_query_cross: float32 [1, 1024, 1024], P(None, 'dp', 'tensor')
- grad_key_cross: float32 [1, 1024, 1024], P(None, 'dp', 'tensor')
- grad_value_cross: float32 [1, 1024, 1024], P(None, 'dp', 'tensor')
- grad_output_cross: float32 [1, 1024, 1024], P(None, 'tensor', 'dp')
- grad_expand: float32 [1, 1024, 4096], P(None, 'dp', 'tensor')
- grad_shrink: float32 [1, 4096, 1024], P(None, 'tensor', 'dp')
- grad_norm_gains: float32 [1, 3, 1024], replicated
- grad_biases: float32 [1, 9, 1024], replicated
- grad_self_out_bias: float32 [1, 1024], replicated
- grad_expand_bias: float32 [1, 4096], replicated
The draws below stay inside these ranges and needn't reach their ends.
Inputs may be any that keep to these rules, and one draw needn't show every extreme that they name: prefix[b] leading tokens of sequence b are seen by every token of it.
All inputs are finite; a program needn't handle non-finite values.
Results may differ from the reference program's by a relative error of at most 0.024.
Values may be sent and summed in bfloat16 or wider, within the bound.
A program may use at most 192 MiB of HBM per device.

```python
import jax
import jax.numpy as jnp
from jax import lax

D = 1024
HEADS = 16
HEAD_DIM = 64
FF = 4096
LAYERS = 1
LEN = 1024
ENC_LEN = 1024
SEQUENCES = 8


def place_ends(values, rng, least, high):
    longest = values.shape.index(max(values.shape))
    spots = []
    for shift in (0, 1):
        where = [jax.random.randint(jax.random.fold_in(rng, axis), (), 0, length) for axis, length in enumerate(values.shape)]
        where[longest] = (where[longest] + shift) % values.shape[longest]
        spots.append(tuple(where))
    return values.at[spots[0]].set(least).at[spots[1]].set(high)


def raised(entries, stream_key, source, target, blocks, factor):
    def block_of(axis_at):
        return (jnp.arange(entries.shape[axis_at]) // (entries.shape[axis_at] // blocks)).reshape((-1,) + (1,) * (entries.ndim - 1 - axis_at))

    near = jax.random.permutation(stream_key, blocks)[block_of(target)]
    other_side = (block_of(target) + blocks // 2) % blocks
    return jnp.where((block_of(source) == near) | (block_of(source) == other_side), factor * entries, entries)


def block_levels(stream_key, dims, cuts, low, high):
    loudness = 1.0
    for axis_at, shards_of in cuts:
        steps = jax.random.uniform(jax.random.fold_in(jax.random.fold_in(stream_key, 6), axis_at), (shards_of,), jnp.float32, low / len(cuts), high / len(cuts))
        loudness = loudness * jnp.repeat(jnp.exp(steps), dims[axis_at] // shards_of).reshape((-1,) + (1,) * (len(dims) - 1 - axis_at))
    return loudness


def noise(stream_key, shape, scale, limit, shards=(), kind=jnp.bfloat16):
    factor_of = block_levels(stream_key, shape, shards, -0.22, 0.18) if shards else 1.0
    drawn = jax.random.normal(stream_key, shape, jnp.float32) * scale * factor_of
    return jnp.minimum(jnp.maximum(drawn, -limit), limit).astype(kind)


def gaussian_with(own_key, shape, deviation, most, pieces, heavy, kind=jnp.bfloat16):
    result = deviation * jax.random.normal(own_key, shape, jnp.float32)
    if pieces:
        result = result * block_levels(own_key, shape, pieces, -0.22, 0.18)
    return jnp.clip(raised(result, jax.random.fold_in(own_key, 3), *heavy), -most, most).astype(kind)


def setup_inputs(seed: int = 0) -> dict:
    seeds = jax.random.split(jax.random.key(seed), 19)
    hidden = noise(seeds[0], (SEQUENCES, LEN, D), 1.0, 6.0, ((0, 8), (1, 4)))
    encoder = noise(seeds[1], (SEQUENCES, ENC_LEN, D), 1.0, 6.0, ((0, 8), (1, 4)))
    prefix = place_ends(jax.random.randint(seeds[2], (SEQUENCES,), LEN // 10, LEN // 2 + 1), jax.random.fold_in(seeds[2], 1), LEN // 10, (LEN // 2 + 1) - 1).astype(jnp.int32)
    query_self = noise(seeds[3], (LAYERS, D, D), D ** -0.5, 0.1875, ((1, 8), (2, 4)))
    key_self = noise(seeds[4], (LAYERS, D, D), D ** -0.5, 0.1875, ((1, 8), (2, 4)))
    value_self = noise(seeds[5], (LAYERS, D, D), D ** -0.5, 0.1875, ((1, 8), (2, 4)))
    output_self = noise(seeds[6], (LAYERS, D, D), (max(1, 4 * D // LEN)) ** -0.5, 3.0, ((1, 4), (2, 8)))
    cross_query_matrix = noise(seeds[7], (LAYERS, D, D), D ** -0.5, 0.1875, ((1, 8), (2, 4)))
    key_cross = noise(seeds[8], (LAYERS, D, D), D ** -0.5, 0.1875, ((1, 8), (2, 4)))
    value_cross = noise(seeds[9], (LAYERS, D, D), D ** -0.5, 0.1875, ((1, 8), (2, 4)))
    output_cross = noise(seeds[10], (LAYERS, D, D), (max(1, 4 * D // ENC_LEN)) ** -0.5, 3.0, ((1, 4), (2, 8)))
    expand = noise(seeds[11], (LAYERS, D, FF), D ** -0.5, 0.1875, ((1, 8), (2, 4)))
    shrink = noise(seeds[12], (LAYERS, FF, D), FF ** -0.5, 0.09375, ((1, 4), (2, 8)))
    norm_gains = jnp.clip(1.0 + 0.15 * jax.random.normal(seeds[13], (LAYERS, 3, D), jnp.float32), 0.25, 1.75)
    biases = noise(seeds[14], (LAYERS, 9, D), 0.3, 1.8, (), jnp.float32)
    self_out_bias = noise(seeds[15], (LAYERS, D), 0.3, 1.8, (), jnp.float32)
    expand_bias = noise(seeds[16], (LAYERS, FF), 0.3, 1.8, (), jnp.float32)
    cotangent = gaussian_with(seeds[17], (SEQUENCES, LEN, D), 1.0, 6.0, ((0, 8), (1, 4)), (0, 2, 8, 2.0))
    return {"hidden": hidden, "encoder": encoder, "prefix": prefix, "query_self": query_self, "key_self": key_self, "value_self": value_self, "output_self": output_self, "cross_query_matrix": cross_query_matrix, "key_cross": key_cross, "value_cross": value_cross, "output_cross": output_cross, "expand": expand, "shrink": shrink, "norm_gains": norm_gains, "biases": biases, "self_out_bias": self_out_bias, "expand_bias": expand_bias, "cotangent": cotangent}


@jax.custom_vjp
def low(v):
    return lax.optimization_barrier(v.astype(jnp.bfloat16)).astype(jnp.float32)

@jax.custom_vjp
def low_back(v):
    return v

def low_keep(v):
    return (low(v), None)

def low_pass(kept, grad):
    return (grad,)

def back_keep(v):
    return (v, None)

def back_low(kept, grad):
    return (low(grad),)
low.defvjp(low_keep, low_pass)
low_back.defvjp(back_keep, back_low)
EPSILON = 1e-05
HIGHEST_LEVEL = lax.Precision.HIGHEST

def rounded_both(values):
    return low_back(low(values))

def project(input_rows, weight_matrix):
    return jnp.einsum('iqa,ax->iqx', input_rows, weight_matrix, precision=HIGHEST_LEVEL)

def post_norm(totals, gain_row, shift_row):
    center = totals - lax.optimization_barrier(jnp.mean(totals, -1, keepdims=True))
    spread = lax.optimization_barrier(jnp.mean(center * center, -1, keepdims=True))
    return center * lax.rsqrt(spread + EPSILON) * gain_row + shift_row

def attend(queries, key_rows, value_rows, allowed):
    scores = low_back(jnp.einsum('qhe,khe->hqk', queries, key_rows, precision=HIGHEST_LEVEL))
    if allowed is not None:
        scores = jnp.where(allowed[None], scores, -1e+30)
    row_max = lax.optimization_barrier(jnp.max(scores, -1, keepdims=True))
    weights = jnp.exp(scores - row_max)
    chances = low(weights / lax.optimization_barrier(jnp.sum(weights, -1, keepdims=True)))
    return jnp.einsum('hqk,khe->qhe', chances, value_rows, precision=HIGHEST_LEVEL)

def self_block(packed):
    queries, key_rows, value_rows, prefix_len = packed
    places = jnp.arange(LEN, dtype=jnp.int32)
    allowed = (places[None, :] <= places[:, None]) | (places[None, :] < prefix_len)
    return attend(queries, key_rows, value_rows, allowed)

def cross_block(packed):
    queries, key_rows, value_rows = packed
    return attend(queries, key_rows, value_rows, None)

def to_heads(values):
    return values.reshape(values.shape[0], values.shape[1], HEADS, HEAD_DIM)

def layer(input_rows, encoder, prefix, weights, gain_rows, bias_row_list, expand_row, self_bias_row):
    query_self, key_self, value_self, output_self, cross_query_matrix, key_cross, value_cross, output_cross, expand, shrink = weights
    scaling = HEAD_DIM ** (-0.5)
    seq_count = input_rows.shape[0]
    inputs_low = low(input_rows)
    queries = rounded_both(to_heads((project(inputs_low, query_self) + bias_row_list[0]) * scaling))
    key_rows = rounded_both(to_heads(project(inputs_low, key_self)))
    value_rows = rounded_both(to_heads(project(inputs_low, value_self) + bias_row_list[1]))
    attended = lax.map(jax.checkpoint(self_block), (queries, key_rows, value_rows, prefix))
    mixed_one = rounded_both(attended.reshape(seq_count, LEN, D))
    branch = low_back(project(mixed_one, output_self))
    normed_one = post_norm(input_rows + branch + self_bias_row, gain_rows[0], bias_row_list[6])
    normed_low = low(normed_one)
    queries_two = rounded_both(to_heads((project(normed_low, cross_query_matrix) + bias_row_list[2]) * scaling))
    keys_two = rounded_both(to_heads(project(encoder, key_cross)))
    values_two = rounded_both(to_heads(project(encoder, value_cross) + bias_row_list[3]))
    attended_two = lax.map(jax.checkpoint(cross_block), (queries_two, keys_two, values_two))
    mixed_two = rounded_both(attended_two.reshape(seq_count, LEN, D))
    branch_two = low_back(project(mixed_two, output_cross))
    normed_two = post_norm(normed_one + branch_two + bias_row_list[4], gain_rows[1], bias_row_list[7])
    pre_active = low_back(project(low(normed_two), expand) + expand_row)
    active = low(jax.nn.gelu(pre_active, approximate=False))
    branch_three = low_back(project(active, shrink))
    return post_norm(normed_two + branch_three + bias_row_list[5], gain_rows[2], bias_row_list[8])

def reference(hidden, encoder, prefix, query_self, key_self, value_self, output_self, cross_query_matrix, key_cross, value_cross, output_cross, expand, shrink, norm_gains, biases, self_out_bias, expand_bias, cotangent):
    matrices = tuple((weight_matrix.astype(jnp.float32) for weight_matrix in (query_self, key_self, value_self, output_self, cross_query_matrix, key_cross, value_cross, output_cross, expand, shrink)))

    def forward(state, encoder_states, weights, gains_all, biases_all, self_all, expand_all):
        for layer_id in range(LAYERS):
            state = layer(state, encoder_states, prefix, tuple((weight_matrix[layer_id] for weight_matrix in weights)), gains_all[layer_id], biases_all[layer_id], expand_all[layer_id], self_all[layer_id])
        return state
    final_state, pullback = jax.vjp(forward, hidden.astype(jnp.float32), encoder.astype(jnp.float32), matrices, norm_gains, biases, self_out_bias, expand_bias)
    grad_state, grad_enc, grad_mats, grad_gains, grad_bias, grad_self, grad_expand = pullback(cotangent.astype(jnp.float32))
    return (final_state.astype(jnp.bfloat16), grad_state, grad_enc, grad_mats[0], grad_mats[1], grad_mats[2], grad_mats[3], grad_mats[4], grad_mats[5], grad_mats[6], grad_mats[7], grad_mats[8], grad_mats[9], grad_gains, grad_bias, grad_self, grad_expand)
```

```python
import functools

import jax
import jax.numpy as jnp
from jax import lax
from jax.experimental import pallas as pl
from jax.experimental.pallas import tpu as pltpu
from jax.sharding import PartitionSpec as P

MESH = pl.DeviceIdType.MESH
BF = jnp.bfloat16
F32 = jnp.float32
EPS = 1e-05
HEAD = 64
LOG2E = 1.4426950408889634
LN2 = 0.6931471805599453
NEG = -1e30
SMALL_ROWS = 24


def dot(a, b, ca, cb):
    return lax.dot_general(a, b, (((ca,), (cb,)), ((), ())), preferred_element_type=F32)


def layer_kernel(nz, sh, *refs):
    (
        prefix,
        hid,
        enc,
        cot,
        wa_in,
        wb_in,
        wc_in,
        we_in,
        ws_in,
        gains,
        biases,
        selfb,
        expb,
        block_out,
        hid_out,
        enc_out,
        ge_out,
        gs_out,
        gc_out,
        ga_out,
        small_out,
        xland,
        eland,
        cland,
        yland,
        zland,
        wa,
        wb,
        wc,
        we,
        ws,
        x1r,
        x2r,
        ct,
        qs,
        ks,
        vs,
        ao,
        q2,
        k2,
        v2,
        a2,
        gg,
        gp,
        n1,
        n2,
        r1,
        r2,
        lse1,
        lse2,
        res,
        sx,
        rx,
        rxd,
        dq,
        do,
        dk,
        dv,
        ksend,
        krecv,
        cs,
        own,
        tmp,
        xt,
        dom,
        qm,
        den,
        outf,
        sm,
        smr,
        smz,
        sems,
    ) = refs
    d = lax.axis_index("dp")
    t = lax.axis_index("tensor")
    x, c = t // 2, t % 2
    z, y = d // 2, d % 2
    nx, nc, ny = 1 - x, 1 - c, 1 - y
    x_dev = (d, nx * 2 + c)
    c_dev = (d, x * 2 + nc)
    y_dev = (z * 2 + ny, t)

    def z_dev(k):
        return (lax.rem(z + k, nz) * 2 + y, t)

    def z_from(k):
        return lax.rem(z + nz - k, nz)

    nq = nz // 4
    rows = hid.shape[0]
    count = [0]

    def new_sem():
        count[0] += 1
        return sems.at[count[0] - 1]

    pending = []

    def send(src, dst, dev):
        cp = pltpu.make_async_remote_copy(
            src_ref=src, dst_ref=dst, send_sem=new_sem(), recv_sem=new_sem(), device_id=dev, device_id_type=MESH
        )
        cp.start()
        pending.append(cp)
        return cp

    def sent(cp):
        cp.wait_send()
        pending[:] = [other for other in pending if other is not cp]

    def local(src, dst):
        cp = pltpu.make_async_copy(src, dst, new_sem())
        cp.start()
        return cp

    barrier = pltpu.get_barrier_semaphore()
    peers = [x_dev, c_dev, y_dev] + [z_dev(k) for k in range(1, nz)]
    for dev in peers:
        pl.semaphore_signal(barrier, inc=1, device_id=dev, device_id_type=MESH)
    pl.semaphore_wait(barrier, len(peers))

    xs = [send(hid, xland.at[x], x_dev)]
    groups = {"a": (wa_in, wa), "b": (wb_in, wb), "c": (wc_in, wc), "e": (we_in, we), "s": (ws_in, ws)}
    zc, yc, cc, lc = {}, {}, {}, {}

    def start_own(g):
        src, buf = groups[g]
        spot = buf.at[c, z, y]
        zc[g] = [send(src, spot, z_dev(k)) for k in range(1, nz)]
        yc[g] = [send(src, spot, y_dev)]
        lc[g] = local(src, spot)

    l_x = local(hid, x1r.at[x])
    l_e = local(enc, x2r.at[x])
    l_c = local(cot, ct.at[x])
    start_own("a")
    start_own("b")
    xs.append(send(enc, eland.at[x], x_dev))
    xs.append(send(cot, ct.at[x], x_dev))
    start_own("c")

    def z_event(g):
        _, buf = groups[g]
        lc[g].wait()
        for k in range(1, nz):
            zc[g][k - 1].wait_recv()
            spot = buf.at[c, z_from(k), y]
            yc[g].append(send(spot, spot, y_dev))
        spot = buf.at[c, :, y]
        cc[g] = [send(spot, spot, c_dev)]

    def y_event(g):
        _, buf = groups[g]
        for cp in yc[g]:
            cp.wait_recv()
        spot = buf.at[c, :, ny]
        cc[g].append(send(spot, spot, c_dev))

    def c_event(g):
        for cp in cc[g]:
            cp.wait_recv()

    def w_all(buf, q, lo, hi):
        return buf[q, :, :, :, lo:hi].reshape(1024, hi - lo)

    def w_rows(buf, q, dn, lo, hi):
        return buf[q, dn * nq : (dn + 1) * nq, :, :, lo:hi].reshape(256, hi - lo)

    def bias_at(ref, row, lo, width):
        return ref[row : row + 1, pl.ds(pl.multiple_of(lo, 256), width)]

    sm[...] = jnp.zeros_like(sm)

    def fold(v):
        return jnp.sum(v.reshape(v.shape[0] // 8, 8, v.shape[1]), axis=0)

    scale = HEAD**-0.5

    l_x.wait()
    xs[0].wait_recv()
    l_xn = local(xland.at[nx], x1r.at[nx])
    z_event("a")
    start_own("e")
    l_xn.wait()
    y_event("a")
    c_event("a")
    for j in range(2):
        xj = x1r[j]
        for q in range(2):
            r = dot(xj, w_all(wa, q, 0, 768), 1, 0)
            lanes = slice(q * 256, q * 256 + 256)
            col = x * 512 + q * 256
            qs[j, :, lanes] = ((r[:, :256] + bias_at(biases, 0, col, 256)) * (scale * LOG2E)).astype(BF)
            ks[2 * j + c, :, lanes] = r[:, 256:512].astype(BF)
            vs[2 * j + c, :, lanes] = (r[:, 512:] + bias_at(biases, 1, col, 256)).astype(BF)
    kv1 = [send(b.at[2 * j + c], b.at[2 * j + c], c_dev) for j in range(2) for b in (ks, vs)]
    xs[1].wait_recv()
    l_en = local(eland.at[nx], x2r.at[nx])
    z_event("b")
    start_own("s")

    lane256 = lax.broadcasted_iota(jnp.int32, (128, 256), 1)
    lane128 = lax.broadcasted_iota(jnp.int32, (128, 128), 1)
    zero_bf = jnp.zeros((128, 256), BF)
    limit = prefix[0]

    def parts_of(keys, causal, j):
        if not causal:
            return [(0, 4, False)]
        return [(0, 2, True)] if j == 0 else [(0, 2, False), (2, 4, True)]

    def scores(qh, k_ref, part, lanes, j, row0):
        b0, b1, masked = part
        k = k_ref[b0:b1, :, lanes].reshape((b1 - b0) * 256, 256)
        s = dot(qh, k, 1, 1)
        if masked:
            cols = b0 * 256 + lax.broadcasted_iota(jnp.int32, s.shape, 1)
            rws = (2 * j + c) * 256 + row0 + lax.broadcasted_iota(jnp.int32, s.shape, 0)
            s = jnp.where((cols <= rws) | (cols < limit), s, NEG)
        return s

    def attend(j, q_ref, k_ref, v_ref, o_ref, l_ref, causal):
        parts = parts_of(k_ref, causal, j)

        def body(i, carry):
            h = i // 2
            row0 = pl.multiple_of((i % 2) * 128, 128)
            rws = pl.ds(row0, 128)
            lanes = pl.ds(pl.multiple_of((h // 4) * 256, 256), 256)
            head = (lane256 // HEAD) == (h % 4)
            qh = jnp.where(head, q_ref[j, rws, lanes], zero_bf)
            ss = [scores(qh, k_ref, p, lanes, j, row0) for p in parts]
            m = functools.reduce(jnp.maximum, [jnp.max(s, axis=1, keepdims=True) for s in ss])
            total = jnp.zeros((128, 1), F32)
            o = jnp.zeros((128, 256), F32)
            for s, (b0, b1, _) in zip(ss, parts):
                p = jnp.exp2(s - m)
                total = total + jnp.sum(p, axis=1, keepdims=True)
                o = o + dot(p.astype(BF), v_ref[b0:b1, :, lanes].reshape((b1 - b0) * 256, 256), 1, 0)
            o = o / total
            o_ref[j, rws, lanes] = jnp.where(head, o.astype(BF), o_ref[j, rws, lanes])
            l_ref[j, rws, :] = jnp.where(lane128 == h, m + jnp.log2(total), l_ref[j, rws, :])
            return carry

        lax.fori_loop(0, 16, body, 0)

    def attend_back(j, q_ref, k_ref, v_ref, o_ref, l_ref, causal):
        parts = parts_of(k_ref, causal, j)
        nk = 256 * parts[-1][1]
        for qt in range(2):
            lanes = slice(qt * 256, qt * 256 + 256)

            def body(i, carry):
                h = i // 2
                row0 = pl.multiple_of((i % 2) * 128, 128)
                rws = pl.ds(row0, 128)
                spot = pl.ds(pl.multiple_of(i * 128, 128), 128)
                head = (lane256 // HEAD) == h
                qh = jnp.where(head, q_ref[j, rws, lanes], zero_bf)
                dh = jnp.where(head, do[rws, lanes], zero_bf)
                delta = jnp.sum(dh.astype(F32) * o_ref[j, rws, lanes].astype(F32), axis=1, keepdims=True)
                lse = jnp.sum(jnp.where(lane128 == h + 4 * qt, l_ref[j, rws, :], 0.0), axis=1, keepdims=True)
                g = jnp.zeros((128, 256), F32)
                for part in parts:
                    b0, b1, _ = part
                    s = scores(qh, k_ref, part, lanes, j, row0)
                    p = jnp.exp2(s - lse)
                    dp = dot(dh, v_ref[b0:b1, :, lanes].reshape((b1 - b0) * 256, 256), 1, 1)
                    ds = (p * (dp - delta)).astype(BF)
                    cs[0, spot, b0 * 256 : b1 * 256] = p.astype(BF)
                    cs[1, spot, b0 * 256 : b1 * 256] = ds
                    g = g + dot(ds, k_ref[b0:b1, :, lanes].reshape((b1 - b0) * 256, 256), 1, 0)
                dq[j, rws, lanes] = jnp.where(head, (g.astype(BF) * scale).astype(BF), dq[j, rws, lanes])
                dom[spot, :] = dh
                qm[spot, :] = qh
                return carry

            lax.fori_loop(0, 8, body, 0)
            for b in range(nk // 256):
                keys = slice(b * 256, b * 256 + 256)
                gv = dot(cs[0, :, keys], dom[...], 0, 0)
                gk = dot(cs[1, :, keys], qm[...], 0, 0) * LN2
                if j == 0:
                    dv[b, :, lanes] = gv
                    dk[b, :, lanes] = gk
                else:
                    dv[b, :, lanes] += gv
                    dk[b, :, lanes] += gk
        if j == 0 and nk < 1024:
            dv[2:4] = jnp.zeros((2, 256, 512), F32)
            dk[2:4] = jnp.zeros((2, 256, 512), F32)

    def project_out(j, src, buf, lo):
        for dn in range(4):
            acc = dot(src[j, :, 0:256], w_rows(buf, 0, dn, lo, lo + 256), 1, 1)
            acc = acc + dot(src[j, :, 256:512], w_rows(buf, 1, dn, lo, lo + 256), 1, 1)
            sx[j, :, dn * 256 : dn * 256 + 256] = acc.astype(BF)

    ex = {}

    def exchange(stage, j):
        ex[stage, j] = send(sx.at[j], rx.at[stage % 2, j], x_dev)

    def arrived(stage, j):
        ex[stage, j].wait_recv()
        sent(ex[stage, j])

    TILE = 32

    def norm_forward(j, stage, base, bias, gain, shift, n_ref, r_ref, low_ref):
        def body(i, carry):
            rws = pl.ds(pl.multiple_of(i * TILE, TILE), TILE)
            v = base[j, rws, :].astype(F32) + sx[j, rws, :].astype(F32) + rx[stage % 2, j, rws, :].astype(F32) + bias
            cen = v - jnp.mean(v, axis=1, keepdims=True)
            r = lax.rsqrt(jnp.mean(cen * cen, axis=1, keepdims=True) + EPS)
            n = cen * r
            o = n * gain + shift
            n_ref[j, rws, :] = n.astype(BF)
            r_ref[j, rws, :] = jnp.broadcast_to(r, (TILE, 128))
            res[j, rws, :] = o
            low_ref[j, rws, :] = o.astype(BF)
            return carry

        lax.fori_loop(0, rows // TILE, body, 0)

    def add_small(row, v):
        sm[row : row + 1, :] += jnp.sum(v, axis=0, keepdims=True) * 0.5

    def back_tile(dz, n, r, gain):
        gz = gain * dz
        ma = jnp.mean(gz, axis=1, keepdims=True)
        mb = jnp.mean(gz * n, axis=1, keepdims=True)
        return (gz - ma - n * mb) * r

    def norm_back(j, stage, gain, n_ref, r_ref, gain_row, shift_row, bias_row):
        def body(i, carry):
            sa, sb, sc = carry
            rws = pl.ds(pl.multiple_of(i * TILE, TILE), TILE)
            dz = res[j, rws, :] + sx[j, rws, :].astype(F32) + rx[stage % 2, j, rws, :].astype(F32)
            n = n_ref[j, rws, :].astype(F32)
            dt = back_tile(dz, n, r_ref[j, rws, 0:1], gain)
            res[j, rws, :] = dt
            ct[j, rws, :] = dt.astype(BF)
            return sa + fold(dz * n), sb + fold(dz), sc + fold(dt)

        zero = jnp.zeros((8, 1024), F32)
        sa, sb, sc = lax.fori_loop(0, rows // TILE, body, (zero, zero, zero))
        add_small(gain_row, sa)
        add_small(shift_row, sb)
        add_small(bias_row, sc)

    for cp in kv1:
        cp.wait_recv()
    attend(0, qs, ks, vs, ao, lse1, True)
    y_event("b")
    attend(1, qs, ks, vs, ao, lse1, True)
    c_event("b")
    project_out(0, ao, wb, 0)
    exchange(0, 0)
    project_out(1, ao, wb, 0)
    exchange(0, 1)
    z_event("c")
    l_e.wait()
    l_en.wait()
    for j in range(2):
        ej = x2r[j]
        for q in range(2):
            r = dot(ej, w_all(wb, q, 256, 768), 1, 0)
            lanes = slice(q * 256, q * 256 + 256)
            k2[2 * j + c, :, lanes] = r[:, :256].astype(BF)
            v2[2 * j + c, :, lanes] = (r[:, 256:] + bias_at(biases, 3, x * 512 + q * 256, 256)).astype(BF)
    kv2 = [send(b.at[2 * j + c], b.at[2 * j + c], c_dev) for j in range(2) for b in (k2, v2)]
    y_event("c")
    for cp in kv2:
        cp.wait_recv()
    c_event("c")

    def cross(j):
        arrived(0, j)
        norm_forward(j, 0, x1r, selfb[0:1, :], gains[0:1, :], biases[6:7, :], n1, r1, x1r)
        xj = x1r[j]
        for q in range(2):
            r = dot(xj, w_all(wc, q, 0, 256), 1, 0) + bias_at(biases, 2, x * 512 + q * 256, 256)
            q2[j, :, q * 256 : q * 256 + 256] = (r * (scale * LOG2E)).astype(BF)
        attend(j, q2, k2, v2, a2, lse2, False)
        project_out(j, a2, wc, 256)
        exchange(1, j)

    cross(0)
    z_event("e")
    cross(1)
    y_event("e")

    root_half = 0.7071067811865476
    norm_pdf = 0.3989422804014327

    def hidden_units(j):
        arrived(1, j)
        norm_forward(j, 1, res, biases[4:5, :], gains[1:2, :], biases[7:8, :], n2, r2, x2r)
        for q in range(2):
            def body(i, carry):
                lanes = pl.ds(pl.multiple_of(i * 256, 256), 256)
                h = dot(x2r[j], we[q, :, :, :, lanes].reshape(1024, 256), 1, 0)
                h = h + expb[0:1, pl.ds(pl.multiple_of(x * 2048 + q * 1024 + i * 256, 256), 256)]
                cdf = 0.5 * (1.0 + lax.erf(h * root_half))
                gg[q, j, :, lanes] = (h * cdf).astype(BF)
                gp[q, j, :, lanes] = (cdf + h * (jnp.exp(-0.5 * h * h) * norm_pdf)).astype(BF)
                return carry

            lax.fori_loop(0, 4, body, 0)

    def units_out(j, src, buf):
        for dn in range(4):
            acc = dot(src[0, j], w_rows(buf, 0, dn, 0, 1024), 1, 1)
            acc = acc + dot(src[1, j], w_rows(buf, 1, dn, 0, 1024), 1, 1)
            sx[j, :, dn * 256 : dn * 256 + 256] = acc.astype(BF)

    c_event("e")
    hidden_units(0)
    z_event("s")
    hidden_units(1)
    y_event("s")
    c_event("s")
    units_out(0, gg, ws)
    exchange(2, 0)
    units_out(1, gg, ws)
    exchange(2, 1)
    l_c.wait()
    xs[2].wait_recv()

    def last_norm(j):
        arrived(2, j)
        gain, shift, bias = gains[2:3, :], biases[8:9, :], biases[5:6, :]

        def body(i, carry):
            sa, sb, sc = carry
            rws = pl.ds(pl.multiple_of(i * TILE, TILE), TILE)
            v = res[j, rws, :] + sx[j, rws, :].astype(F32) + rx[0, j, rws, :].astype(F32) + bias
            cen = v - jnp.mean(v, axis=1, keepdims=True)
            r = lax.rsqrt(jnp.mean(cen * cen, axis=1, keepdims=True) + EPS)
            n = cen * r
            xt[rws, :] = (n * gain + shift).astype(BF)
            dz = ct[j, rws, :].astype(F32)
            dt = back_tile(dz, n, r, gain)
            res[j, rws, :] = dt
            ct[j, rws, :] = dt.astype(BF)
            return sa + fold(dz * n), sb + fold(dz), sc + fold(dt)

        zero = jnp.zeros((8, 1024), F32)
        sa, sb, sc = lax.fori_loop(0, rows // TILE, body, (zero, zero, zero))
        add_small(2, sa)
        add_small(11, sb)
        add_small(8, sc)

        @pl.when(x == j)
        def _():
            local(xt, block_out).wait()

    def units_back(j):
        for q in range(2):
            def body(i, carry):
                lanes = pl.ds(pl.multiple_of(i * 256, 256), 256)
                g = dot(ct[j], ws[q, :, :, :, lanes].reshape(1024, 256), 1, 0)
                g = (g * gp[q, j, :, lanes].astype(F32)).astype(BF)
                gp[q, j, :, lanes] = g
                sm[pl.ds(13 + 2 * x + q, 1), lanes] += jnp.sum(g.astype(F32), axis=0, keepdims=True)
                return carry

            lax.fori_loop(0, 4, body, 0)
        units_out(j, gp, we)
        exchange(3, j)

    last_norm(0)
    units_back(0)
    last_norm(1)
    units_back(1)

    def grad_into(dst, pieces):
        def body(i, carry):
            lanes = pl.ds(pl.multiple_of(i * 256, 256), 256)
            lo = 0
            for left, right in pieces:
                g = dot(left[:, :, lanes].reshape(512, 256), right, 0, 0)
                w = g.shape[1]
                dst[pl.ds(i * nq, nq), :, :, lo : lo + w] = g.astype(BF).reshape(nq, 2, sh, w)
                lo += w
            return carry

        lax.fori_loop(0, 4, body, 0)

    gsend = {}
    gy, gz_ = {}, {}

    own_of = {0: own.at[0], 1: own.at[1], 2: we.at[0], 3: we.at[1]}
    send_of = {2: ws.at[0], 3: ws.at[1]}

    def unit_pair(ref, q):
        return ref[q].reshape(512, 1024)

    for g in ("e", "s"):
        for cp in zc[g] + yc[g] + cc[g]:
            sent(cp)
    es_send = [ws.at[0], ws.at[1]]
    grad_into(es_send[0], [(x2r, unit_pair(gp, nc))])
    gsend[0] = send(es_send[0], cland.at[0], c_dev)
    grad_into(es_send[1], [(ct, unit_pair(gg, nc))])
    gsend[1] = send(es_send[1], cland.at[1], c_dev)
    grad_into(own_of[0], [(x2r, unit_pair(gp, c))])
    grad_into(own_of[1], [(ct, unit_pair(gg, c))])
    l_en2a = local(enc, x2r.at[x])
    l_en2b = local(eland.at[nx], x2r.at[nx])


    def grad_core(g):
        gsend[g].wait_recv()
        local(cland.at[g], tmp).wait()
        o = own_of[g]

        def body(i, carry):
            blk = pl.ds(i * nq, nq)
            o[blk] = (o[blk].astype(F32) + tmp[blk].astype(F32)).astype(BF)
            return carry

        lax.fori_loop(0, 4, body, 0)
        gy[g] = send(o.at[:, ny], yland.at[g], y_dev)

    def grad_y(g):
        gy[g].wait_recv()
        local(yland.at[g], tmp.at[:, 0]).wait()
        o = own_of[g]

        def body(i, carry):
            blk = pl.ds(i * nq, nq)
            o[blk, y] = (o[blk, y].astype(F32) + tmp[blk, 0].astype(F32)).astype(BF)
            return carry

        lax.fori_loop(0, 4, body, 0)
        gz_[g] = [send(o.at[lax.rem(z + k, nz), y], zland.at[g, k], z_dev(k)) for k in range(1, nz)]

    def grad_z(g, out):
        cps = []
        for k in range(1, nz):
            gz_[g][k - 1].wait_recv()
            cps.append(local(zland.at[g, k], tmp.at[k, 0]))
        for cp in cps:
            cp.wait()
        acc = own_of[g][z, y].astype(F32)
        for k in range(1, nz):
            acc = acc + tmp[k, 0].astype(F32)
        outf[...] = acc
        local(outf, out).wait()

    def sum_rows(row, src, col):
        sm[row : row + 1, pl.ds(pl.multiple_of(col, 256), 256)] += jnp.sum(src.astype(F32), axis=0, keepdims=True)

    def heads_back(j, buf, lo, q_ref, k_ref, v_ref, o_ref, l_ref, causal):
        for q in range(2):
            do[:, q * 256 : q * 256 + 256] = dot(ct[j], w_all(buf, q, lo, lo + 256), 1, 0).astype(BF)
        attend_back(j, q_ref, k_ref, v_ref, o_ref, l_ref, causal)

    def swap_kv(slot):
        for j in range(2):
            ksend[0, j] = dk[2 * j + nc].astype(BF)
            ksend[1, j] = dv[2 * j + nc].astype(BF)
        return send(ksend, krecv.at[slot], c_dev)

    def join_kv(slot):
        for j in range(2):
            krecv[slot, 0, j] = (dk[2 * j + c] + krecv[slot, 0, j].astype(F32)).astype(BF)
            krecv[slot, 1, j] = (dv[2 * j + c] + krecv[slot, 1, j].astype(F32)).astype(BF)

    def head_cols(ref, q):
        return ref[:, :, pl.ds(pl.multiple_of(q * 256, 256), 256)].reshape(512, 256)

    def cross_back(j):
        arrived(3, j)
        norm_back(j, 3, gains[1:2, :], n2, r2, 1, 10, 7)
        heads_back(j, wc, 256, q2, k2, v2, a2, lse2, False)
        for dn in range(4):
            acc = dot(dq[j, :, 0:256], w_rows(wc, 0, dn, 0, 256), 1, 1)
            acc = acc + dot(dq[j, :, 256:512], w_rows(wc, 1, dn, 0, 256), 1, 1)
            sx[j, :, dn * 256 : dn * 256 + 256] = acc.astype(BF)
        exchange(4, j)

    cross_back(0)
    grad_core(0)
    cross_back(1)
    grad_core(1)
    swap2 = swap_kv(0)
    for j in range(2):
        for q in range(2):
            sum_rows(5, dq[j, :, q * 256 : q * 256 + 256], x * 512 + q * 256)
    grad_y(0)
    swap2.wait_recv()
    join_kv(0)
    for j in range(2):
        for q in range(2):
            sum_rows(6, krecv[0, 1, j, :, q * 256 : q * 256 + 256], x * 512 + q * 256)
    l_en2a.wait()
    l_en2b.wait()

    def cross_pieces(q):
        return [
            (ct, head_cols(a2, q)),
            (x1r, head_cols(dq, q)),
            (x2r, head_cols(krecv.at[0, 0], q)),
            (x2r, head_cols(krecv.at[0, 1], q)),
        ]

    sent(gsend[0])
    grad_into(send_of[2], cross_pieces(nc))
    gsend[2] = send(send_of[2], cland.at[2], c_dev)
    grad_into(own_of[2], cross_pieces(c))
    l_x2a = local(hid, x1r.at[x])
    l_x2b = local(xland.at[nx], x1r.at[nx])

    def input_part(j, terms, dn):
        acc = None
        for ref, buf, lo in terms:
            for q in range(2):
                part = dot(ref[j, :, q * 256 : q * 256 + 256], w_rows(buf, q, dn, lo, lo + 256), 1, 1)
                acc = part if acc is None else acc + part
        return acc

    enc_terms = [(krecv.at[0, 0], wb, 256), (krecv.at[0, 1], wb, 512)]
    for dn in range(4):
        cols = slice(dn * 256, dn * 256 + 256)
        xt[:, cols] = input_part(nx, enc_terms, dn).astype(BF)
    for dn in range(4):
        cols = slice(dn * 256, dn * 256 + 256)
        den[:, cols] = input_part(x, enc_terms, dn)
    enc_x = send(xt, rxd.at[0], x_dev)

    def self_back(j):
        arrived(4, j)
        norm_back(j, 4, gains[0:1, :], n1, r1, 0, 9, 12)
        heads_back(j, wb, 0, qs, ks, vs, ao, lse1, True)

    self_back(0)
    sent(enc_x)
    grad_y(1)
    grad_core(2)
    self_back(1)
    sent(swap2)
    swap1 = swap_kv(1)
    for j in range(2):
        for q in range(2):
            sum_rows(3, dq[j, :, q * 256 : q * 256 + 256], x * 512 + q * 256)
    grad_y(2)
    swap1.wait_recv()
    join_kv(1)
    for j in range(2):
        for q in range(2):
            sum_rows(4, krecv[1, 1, j, :, q * 256 : q * 256 + 256], x * 512 + q * 256)
    l_x2a.wait()
    l_x2b.wait()

    s1 = send(sm, smr.at[0], c_dev)

    def self_pieces(q):
        return [
            (ct, head_cols(ao, q)),
            (x1r, head_cols(dq, q)),
            (x1r, head_cols(krecv.at[1, 0], q)),
            (x1r, head_cols(krecv.at[1, 1], q)),
        ]

    sent(gsend[1])
    grad_into(send_of[3], self_pieces(nc))
    gsend[3] = send(send_of[3], cland.at[3], c_dev)
    in_terms = [(dq, wa, 0), (krecv.at[1, 0], wa, 256), (krecv.at[1, 1], wa, 512)]
    for dn in range(4):
        cols = slice(dn * 256, dn * 256 + 256)
        xt[:, cols] = input_part(nx, in_terms, dn).astype(BF)
    hid_x = send(xt, rxd.at[1], x_dev)
    grad_into(own_of[3], self_pieces(c))
    for dn in range(4):
        cols = slice(dn * 256, dn * 256 + 256)
        res[x, :, cols] += input_part(x, in_terms, dn)
    s1.wait_recv()
    sent(s1)
    sm[...] += smr[0]
    s2 = send(sm, smr.at[1], x_dev)
    sent(hid_x)
    grad_core(3)
    s2.wait_recv()
    sent(s2)
    sm[...] += smr[1]
    s3 = send(sm, smr.at[2], y_dev)
    grad_z(0, ge_out)
    s3.wait_recv()
    sent(s3)
    sm[...] += smr[2]
    smz[z] = sm[...]
    s4 = [send(sm, smz.at[z], z_dev(k)) for k in range(1, nz)]
    grad_z(1, gs_out)
    enc_x.wait_recv()
    den[...] += rxd[0].astype(F32)
    o1 = local(den, enc_out)
    hid_x.wait_recv()
    res[x] += rxd[1].astype(F32)
    o2 = local(res.at[x], hid_out)
    grad_z(2, gc_out)
    for cp in s4:
        cp.wait_recv()
        sent(cp)
    acc = smz[0]
    for k in range(1, nz):
        acc = acc + smz[k]
    sm[...] = acc
    o3 = local(sm, small_out)
    grad_y(3)
    grad_z(3, ga_out)
    for cp in (o1, o2, o3):
        cp.wait()
    for cp in list(pending):
        sent(cp)


def run_layer(nz, sh, prefix, hid, enc, cot, shards, gains, biases, selfb, expb):
    any_spec = pl.BlockSpec(memory_space=pl.ANY)
    vmem = pl.BlockSpec(memory_space=pltpu.VMEM)
    rows = hid.shape[0]
    shape = jax.ShapeDtypeStruct
    outs = [
        shape((rows, 1024), BF),
        shape((rows, 1024), F32),
        shape((rows, 1024), F32),
        shape((sh, 1024), F32),
        shape((sh, 1024), F32),
        shape((sh, 1024), F32),
        shape((sh, 1024), F32),
        shape((SMALL_ROWS, 1024), F32),
        shape((2, rows, 1024), BF),
        shape((2, rows, 1024), BF),
        shape((4, nz, 2, sh, 1024), BF),
        shape((4, nz, sh, 1024), BF),
        shape((4, nz, sh, 1024), BF),
    ]

    def weight(n):
        return pltpu.VMEM((2, nz, 2, sh, n), BF)

    def acts(n, kind=BF):
        return pltpu.VMEM((2, rows, n), kind)

    def keys(kind=BF):
        return pltpu.VMEM((4, rows, 512), kind)

    scratch = [
        weight(768),
        weight(768),
        weight(512),
        weight(1024),
        weight(1024),
        acts(1024),
        acts(1024),
        acts(1024),
        acts(512),
        keys(),
        keys(),
        acts(512),
        acts(512),
        keys(),
        keys(),
        acts(512),
        pltpu.VMEM((2, 2, rows, 1024), BF),
        pltpu.VMEM((2, 2, rows, 1024), BF),
        acts(1024),
        acts(1024),
        acts(128, F32),
        acts(128, F32),
        acts(128, F32),
        acts(128, F32),
        acts(1024, F32),
        acts(1024),
        pltpu.VMEM((2, 2, rows, 1024), BF),
        acts(1024),
        acts(512),
        pltpu.VMEM((rows, 512), BF),
        keys(F32),
        keys(F32),
        pltpu.VMEM((2, 2, rows, 512), BF),
        pltpu.VMEM((2, 2, 2, rows, 512), BF),
        pltpu.VMEM((2, 1024, 1024), BF),
        pltpu.VMEM((2, nz, 2, sh, 1024), BF),
        pltpu.VMEM((nz, 2, sh, 1024), BF),
        pltpu.VMEM((rows, 1024), BF),
        pltpu.VMEM((1024, 256), BF),
        pltpu.VMEM((1024, 256), BF),
        pltpu.VMEM((rows, 1024), F32),
        pltpu.VMEM((sh, 1024), F32),
        pltpu.VMEM((SMALL_ROWS, 1024), F32),
        pltpu.VMEM((3, SMALL_ROWS, 1024), F32),
        pltpu.VMEM((nz, SMALL_ROWS, 1024), F32),
        pltpu.SemaphoreType.DMA((200 + 40 * nz,)),
    ]
    return pl.pallas_call(
        functools.partial(layer_kernel, nz, sh),
        out_shape=outs,
        in_specs=[pl.BlockSpec(memory_space=pltpu.SMEM)] + [any_spec] * 8 + [vmem] * 4,
        out_specs=[any_spec] * len(outs),
        scratch_shapes=scratch,
        compiler_params=pltpu.CompilerParams(
            collective_id=0, has_side_effects=True, vmem_limit_bytes=67043328
        ),
    )(prefix, hid, enc, cot, *shards, gains, biases, selfb, expb)


def per_device(
    hidden,
    encoder,
    prefix,
    query_self,
    key_self,
    value_self,
    output_self,
    cross_query_matrix,
    key_cross,
    value_cross,
    output_cross,
    expand,
    shrink,
    norm_gains,
    biases,
    self_out_bias,
    expand_bias,
    cotangent,
):
    sh = query_self.shape[1]
    nz = 1024 // sh // 2
    shards = (
        jnp.concatenate([query_self[0], key_self[0], value_self[0]], axis=1),
        jnp.concatenate([output_self[0].T, key_cross[0], value_cross[0]], axis=1),
        jnp.concatenate([cross_query_matrix[0], output_cross[0].T], axis=1),
        expand[0],
        shrink[0].T,
    )
    outs = run_layer(
        nz,
        sh,
        prefix,
        hidden[0],
        encoder[0],
        cotangent[0],
        shards,
        norm_gains[0],
        biases[0],
        self_out_bias,
        expand_bias,
    )
    block, grad_hid, grad_enc, ge, gs, gc, ga, small = outs[:8]

    def part(g, i):
        return g[:, i * 256 : i * 256 + 256]

    return (
        block[None],
        grad_hid[None],
        grad_enc[None],
        part(ga, 1)[None],
        part(ga, 2)[None],
        part(ga, 3)[None],
        part(ga, 0).T[None],
        part(gc, 1)[None],
        part(gc, 2)[None],
        part(gc, 3)[None],
        part(gc, 0).T[None],
        ge[None],
        gs.T[None],
        small[0:3][None],
        small[3:12][None],
        small[12:13],
        small[13:17].reshape(1, 4096),
    )


def solution(mesh):
    in_specs = (
        P("dp", "tensor", None),
        P("dp", "tensor", None),
        P("dp"),
        P(None, "dp", "tensor"),
        P(None, "dp", "tensor"),
        P(None, "dp", "tensor"),
        P(None, "tensor", "dp"),
        P(None, "dp", "tensor"),
        P(None, "dp", "tensor"),
        P(None, "dp", "tensor"),
        P(None, "tensor", "dp"),
        P(None, "dp", "tensor"),
        P(None, "tensor", "dp"),
        P(),
        P(),
        P(),
        P(),
        P("dp", "tensor", None),
    )
    out_specs = (
        P("dp", "tensor", None),
        P("dp", "tensor", None),
        P("dp", "tensor", None),
        P(None, "dp", "tensor"),
        P(None, "dp", "tensor"),
        P(None, "dp", "tensor"),
        P(None, "tensor", "dp"),
        P(None, "dp", "tensor"),
        P(None, "dp", "tensor"),
        P(None, "dp", "tensor"),
        P(None, "tensor", "dp"),
        P(None, "dp", "tensor"),
        P(None, "tensor", "dp"),
        P(),
        P(),
        P(),
        P(),
    )
    return jax.shard_map(
        per_device, mesh=mesh, in_specs=in_specs, out_specs=out_specs, check_vma=False
    )
```

```python
import functools

import jax
import jax.numpy as jnp
from jax import lax
from jax.experimental import pallas as pl
from jax.experimental.pallas import tpu as pltpu
from jax.sharding import PartitionSpec as P

MESH = pl.DeviceIdType.MESH
BF = jnp.bfloat16
F32 = jnp.float32
EPS = 1e-05
HEAD = 64
LOG2E = 1.4426950408889634
LN2 = 0.6931471805599453
NEG = -1e30
SMALL_ROWS = 24


def dot(a, b, ca, cb):
    return lax.dot_general(a, b, (((ca,), (cb,)), ((), ())), preferred_element_type=F32)


def layer_kernel(nz, sh, *refs):
    (
        prefix,
        hid,
        enc,
        cot,
        wa_in,
        wb_in,
        wc_in,
        we_in,
        ws_in,
        gains,
        biases,
        selfb,
        expb,
        block_out,
        hid_out,
        enc_out,
        ge_out,
        gs_out,
        gc_out,
        ga_out,
        small_out,
        xland,
        eland,
        cland,
        yland,
        zland,
        wa,
        wb,
        wc,
        we,
        ws,
        x1r,
        x2r,
        ct,
        qs,
        ks,
        vs,
        ao,
        q2,
        k2,
        v2,
        a2,
        gg,
        gp,
        n1,
        n2,
        r1,
        r2,
        lse1,
        lse2,
        res,
        sx,
        rx,
        rxd,
        dq,
        do,
        dk,
        dv,
        ksend,
        krecv,
        cs,
        own,
        tmp,
        xt,
        dom,
        qm,
        den,
        outf,
        sm,
        smr,
        smz,
        sems,
    ) = refs
    d = lax.axis_index("dp")
    t = lax.axis_index("tensor")
    x, c = t // 2, t % 2
    z, y = d // 2, d % 2
    nx, nc, ny = 1 - x, 1 - c, 1 - y
    x_dev = (d, nx * 2 + c)
    c_dev = (d, x * 2 + nc)
    y_dev = (z * 2 + ny, t)

    def z_dev(k):
        return (lax.rem(z + k, nz) * 2 + y, t)

    def z_from(k):
        return lax.rem(z + nz - k, nz)

    nq = nz // 4
    rows = hid.shape[0]
    count = [0]

    def new_sem():
        count[0] += 1
        return sems.at[count[0] - 1]

    pending = []

    def plan(src, dst, dev):
        return pltpu.make_async_remote_copy(
            src_ref=src, dst_ref=dst, send_sem=new_sem(), recv_sem=new_sem(), device_id=dev, device_id_type=MESH
        )

    def launch(cp):
        cp.start()
        pending.append(cp)
        return cp

    def send(src, dst, dev):
        return launch(plan(src, dst, dev))

    def sent(cp):
        cp.wait_send()
        pending[:] = [other for other in pending if other is not cp]

    def local(src, dst):
        cp = pltpu.make_async_copy(src, dst, new_sem())
        cp.start()
        return cp

    barrier = pltpu.get_barrier_semaphore()
    peers = [x_dev, c_dev, y_dev] + [z_dev(k) for k in range(1, nz)]
    for dev in peers:
        pl.semaphore_signal(barrier, inc=1, device_id=dev, device_id_type=MESH)
    pl.semaphore_wait(barrier, len(peers))

    xs = [send(hid, xland.at[x], x_dev)]
    groups = {"a": (wa_in, wa), "b": (wb_in, wb), "c": (wc_in, wc), "e": (we_in, we), "s": (ws_in, ws)}
    zc, yc, cz, cy, lc = {}, {}, {}, {}, {}
    peers_z = range(1, nz)

    for g in groups:
        src, buf = groups[g]
        spot = buf.at[c, z, y]
        zc[g] = {k: plan(src, spot, z_dev(k)) for k in peers_z}
        yc[g] = {0: plan(src, spot, y_dev)}
        cz[g] = {0: plan(src, spot, c_dev)}
        cy[g] = {}
        for k in range(nz):
            zk = z_from(k)
            if k:
                spot = buf.at[c, zk, y]
                yc[g][k] = plan(spot, spot, y_dev)
                cz[g][k] = plan(spot, spot, c_dev)
            spot = buf.at[c, zk, ny]
            cy[g][k] = plan(spot, spot, c_dev)

    def start_z(g):
        for k in peers_z:
            launch(zc[g][k])

    def start_y(g):
        launch(yc[g][0])

    def start_c(g):
        src, buf = groups[g]
        launch(cz[g][0])
        lc[g] = local(src, buf.at[c, z, y])

    def thirds(part):
        return range(1 + (nz - 1) * part // 3, 1 + (nz - 1) * (part + 1) // 3)

    def z_event(g, part):
        for k in thirds(part):
            zc[g][k].wait_recv()
            launch(yc[g][k])
            launch(cz[g][k])

    def y_event(g, part):
        for k in [0] if part < 0 else thirds(part):
            yc[g][k].wait_recv()
            launch(cy[g][k])

    def c_event(g):
        lc[g].wait()
        for cp in list(cz[g].values()) + list(cy[g].values()):
            cp.wait_recv()

    def run(*words):
        for word in words:
            kind, g, part = word[0], word[1], int(word[2:] or 0)
            if kind == "o":
                start_y(g)
            else:
                (z_event if kind == "z" else y_event)(g, part)

    start_z("a")
    start_y("a")
    start_c("a")
    l_x = local(hid, x1r.at[x])
    l_e = local(enc, x2r.at[x])
    l_c = local(cot, ct.at[x])
    start_z("b")
    start_y("b")
    start_c("b")
    xs.append(send(enc, eland.at[x], x_dev))
    xs.append(send(cot, ct.at[x], x_dev))
    for g in ("c", "e", "s"):
        start_z(g)
        start_c(g)

    def hooked(hooks, i):
        for at, text in hooks.items():
            if isinstance(text, tuple):
                pl.when(i == at // 2 * 2)(functools.partial(run, *text))
            else:
                pl.when(i == at // 2 * 2)(text)

    def w_all(buf, q, lo, hi):
        return buf[q, :, :, :, lo:hi].reshape(1024, hi - lo)

    def w_rows(buf, q, dn, lo, hi):
        return buf[q, dn * nq : (dn + 1) * nq, :, :, lo:hi].reshape(256, hi - lo)

    def bias_at(ref, row, lo, width):
        return ref[row : row + 1, pl.ds(pl.multiple_of(lo, 256), width)]

    sm[...] = jnp.zeros_like(sm)

    def fold(v):
        return jnp.sum(v.reshape(v.shape[0] // 8, 8, v.shape[1]), axis=0)

    scale = HEAD**-0.5

    l_x.wait()
    xs[0].wait_recv()
    l_xn = local(xland.at[nx], x1r.at[nx])
    run("za0", "ya-1", "za1", "ya0", "za2", "oc", "ya1", "ya2")
    l_xn.wait()
    c_event("a")
    kv1 = []
    for j in range(2):
        xj = x1r[j]
        for q in range(2):
            r = dot(xj, w_all(wa, q, 0, 768), 1, 0)
            lanes = slice(q * 256, q * 256 + 256)
            col = x * 512 + q * 256
            qs[j, :, lanes] = ((r[:, :256] + bias_at(biases, 0, col, 256)) * (scale * LOG2E)).astype(BF)
            ks[2 * j + c, :, lanes] = r[:, 256:512].astype(BF)
            vs[2 * j + c, :, lanes] = (r[:, 512:] + bias_at(biases, 1, col, 256)).astype(BF)
        kv1 += [send(b.at[2 * j + c], b.at[2 * j + c], c_dev) for b in (ks, vs)]
        run(*(("zb0", "oe") if j == 0 else ("zb1",)))
    xs[1].wait_recv()
    l_en = local(eland.at[nx], x2r.at[nx])

    lane256 = lax.broadcasted_iota(jnp.int32, (128, 256), 1)
    lane128 = lax.broadcasted_iota(jnp.int32, (128, 128), 1)
    zero_bf = jnp.zeros((128, 256), BF)
    lane256w = lax.broadcasted_iota(jnp.int32, (256, 256), 1)
    lane128w = lax.broadcasted_iota(jnp.int32, (256, 128), 1)
    zero_bfw = jnp.zeros((256, 256), BF)
    limit = prefix[0]

    def parts_of(keys, causal, j):
        if not causal:
            return [(0, 4, False)]
        return [(0, 2, True)] if j == 0 else [(0, 2, False), (2, 4, True)]

    def scores(qh, k_ref, part, lanes, j, row0):
        b0, b1, masked = part
        k = k_ref[b0:b1, :, lanes].reshape((b1 - b0) * 256, 256)
        s = dot(qh, k, 1, 1)
        if masked:
            cols = b0 * 256 + lax.broadcasted_iota(jnp.int32, s.shape, 1)
            rws = (2 * j + c) * 256 + row0 + lax.broadcasted_iota(jnp.int32, s.shape, 0)
            s = jnp.where((cols <= rws) | (cols < limit), s, NEG)
        return s

    def attend(j, q_ref, k_ref, v_ref, o_ref, l_ref, causal, hooks):
        parts = parts_of(k_ref, causal, j)

        def body(i, carry):
            hooked(hooks, 2 * i)
            h = i
            row0 = 0
            rws = slice(0, 256)
            lanes = pl.ds(pl.multiple_of((h // 4) * 256, 256), 256)
            head = (lane256w // HEAD) == (h % 4)
            qh = jnp.where(head, q_ref[j, rws, lanes], zero_bfw)
            ss = [scores(qh, k_ref, p, lanes, j, row0) for p in parts]
            m = functools.reduce(jnp.maximum, [jnp.max(s, axis=1, keepdims=True) for s in ss])
            total = jnp.zeros((256, 1), F32)
            o = jnp.zeros((256, 256), F32)
            for s, (b0, b1, _) in zip(ss, parts):
                p = jnp.exp2(s - m)
                total = total + jnp.sum(p, axis=1, keepdims=True)
                o = o + dot(p.astype(BF), v_ref[b0:b1, :, lanes].reshape((b1 - b0) * 256, 256), 1, 0)
            o = o / total
            o_ref[j, rws, lanes] = jnp.where(head, o.astype(BF), o_ref[j, rws, lanes])
            l_ref[j, rws, :] = jnp.where(lane128w == h, m + jnp.log2(total), l_ref[j, rws, :])
            return carry

        lax.fori_loop(0, 8, body, 0)

    def attend_back(j, q_ref, k_ref, v_ref, o_ref, l_ref, causal, hooks):
        parts = parts_of(k_ref, causal, j)
        nk = 256 * parts[-1][1]
        for qt in range(2):
            lanes = slice(qt * 256, qt * 256 + 256)

            def body(i, carry):
                hooked(hooks[qt], 2 * i)
                h = i
                row0 = 0
                rws = slice(0, 256)
                spot = pl.ds(pl.multiple_of(i * 256, 256), 256)
                head = (lane256w // HEAD) == h
                qh = jnp.where(head, q_ref[j, rws, lanes], zero_bfw)
                dh = jnp.where(head, do[rws, lanes], zero_bfw)
                delta = jnp.sum(dh.astype(F32) * o_ref[j, rws, lanes].astype(F32), axis=1, keepdims=True)
                lse = jnp.sum(jnp.where(lane128w == h + 4 * qt, l_ref[j, rws, :], 0.0), axis=1, keepdims=True)
                g = jnp.zeros((256, 256), F32)
                for part in parts:
                    b0, b1, _ = part
                    s = scores(qh, k_ref, part, lanes, j, row0)
                    p = jnp.exp2(s - lse)
                    dp = dot(dh, v_ref[b0:b1, :, lanes].reshape((b1 - b0) * 256, 256), 1, 1)
                    ds = (p * (dp - delta)).astype(BF)
                    cs[0, spot, b0 * 256 : b1 * 256] = p.astype(BF)
                    cs[1, spot, b0 * 256 : b1 * 256] = ds
                    g = g + dot(ds, k_ref[b0:b1, :, lanes].reshape((b1 - b0) * 256, 256), 1, 0)
                dq[j, rws, lanes] = jnp.where(head, (g.astype(BF) * scale).astype(BF), dq[j, rws, lanes])
                dom[spot, :] = dh
                qm[spot, :] = qh
                return carry

            lax.fori_loop(0, 4, body, 0)
            for b in range(nk // 256):
                keys = slice(b * 256, b * 256 + 256)
                gv = dot(cs[0, :, keys], dom[...], 0, 0)
                gk = dot(cs[1, :, keys], qm[...], 0, 0) * LN2
                if j == 0:
                    dv[b, :, lanes] = gv
                    dk[b, :, lanes] = gk
                else:
                    dv[b, :, lanes] += gv
                    dk[b, :, lanes] += gk
        if j == 0 and nk < 1024:
            dv[2:4] = jnp.zeros((2, 256, 512), F32)
            dk[2:4] = jnp.zeros((2, 256, 512), F32)

    def project_out(j, src, buf, lo):
        for dn in range(4):
            acc = dot(src[j, :, 0:256], w_rows(buf, 0, dn, lo, lo + 256), 1, 1)
            acc = acc + dot(src[j, :, 256:512], w_rows(buf, 1, dn, lo, lo + 256), 1, 1)
            sx[j, :, dn * 256 : dn * 256 + 256] = acc.astype(BF)

    ex = {}

    def exchange(stage, j):
        ex[stage, j] = send(sx.at[j], rx.at[stage % 2, j], x_dev)

    def arrived(stage, j):
        ex[stage, j].wait_recv()
        sent(ex[stage, j])

    TILE = 32

    def norm_forward(j, stage, base, bias, gain, shift, n_ref, r_ref, low_ref):
        def body(i, carry):
            rws = pl.ds(pl.multiple_of(i * TILE, TILE), TILE)
            v = base[j, rws, :].astype(F32) + sx[j, rws, :].astype(F32) + rx[stage % 2, j, rws, :].astype(F32) + bias
            cen = v - jnp.mean(v, axis=1, keepdims=True)
            r = lax.rsqrt(jnp.mean(cen * cen, axis=1, keepdims=True) + EPS)
            n = cen * r
            o = n * gain + shift
            n_ref[j, rws, :] = n.astype(BF)
            r_ref[j, rws, :] = jnp.broadcast_to(r, (TILE, 128))
            res[j, rws, :] = o
            low_ref[j, rws, :] = o.astype(BF)
            return carry

        lax.fori_loop(0, rows // TILE, body, 0)

    def add_small(row, v):
        sm[row : row + 1, :] += jnp.sum(v, axis=0, keepdims=True) * 0.5

    def back_tile(dz, n, r, gain):
        gz = gain * dz
        ma = jnp.mean(gz, axis=1, keepdims=True)
        mb = jnp.mean(gz * n, axis=1, keepdims=True)
        return (gz - ma - n * mb) * r

    def norm_back(j, stage, gain, n_ref, r_ref, gain_row, shift_row, bias_row):
        def body(i, carry):
            sa, sb, sc = carry
            rws = pl.ds(pl.multiple_of(i * TILE, TILE), TILE)
            dz = res[j, rws, :] + sx[j, rws, :].astype(F32) + rx[stage % 2, j, rws, :].astype(F32)
            n = n_ref[j, rws, :].astype(F32)
            dt = back_tile(dz, n, r_ref[j, rws, 0:1], gain)
            res[j, rws, :] = dt
            ct[j, rws, :] = dt.astype(BF)
            return sa + fold(dz * n), sb + fold(dz), sc + fold(dt)

        zero = jnp.zeros((8, 1024), F32)
        sa, sb, sc = lax.fori_loop(0, rows // TILE, body, (zero, zero, zero))
        add_small(gain_row, sa)
        add_small(shift_row, sb)
        add_small(bias_row, sc)

    for cp in kv1:
        cp.wait_recv()
    attend(0, qs, ks, vs, ao, lse1, True, {5: ("zb2",), 14: ("zc0", "os",)})
    run("yb-1", "yb0", "yb1", "zc1", "yb2")
    c_event("b")
    project_out(0, ao, wb, 0)
    exchange(0, 0)
    attend(1, qs, ks, vs, ao, lse1, True, {4: ("zc2",), 13: ("yc-1", "yc0",)})
    project_out(1, ao, wb, 0)
    exchange(0, 1)
    run("ze0", "yc1", "yc2")
    l_e.wait()
    l_en.wait()
    for j in range(2):
        ej = x2r[j]
        for q in range(2):
            r = dot(ej, w_all(wb, q, 256, 768), 1, 0)
            lanes = slice(q * 256, q * 256 + 256)
            k2[2 * j + c, :, lanes] = r[:, :256].astype(BF)
            v2[2 * j + c, :, lanes] = (r[:, 256:] + bias_at(biases, 3, x * 512 + q * 256, 256)).astype(BF)
    kv2 = [send(b.at[2 * j + c], b.at[2 * j + c], c_dev) for j in range(2) for b in (k2, v2)]
    c_event("c")
    for cp in kv2:
        cp.wait_recv()

    def cross(j, hooks):
        arrived(0, j)
        norm_forward(j, 0, x1r, selfb[0:1, :], gains[0:1, :], biases[6:7, :], n1, r1, x1r)
        xj = x1r[j]
        for q in range(2):
            r = dot(xj, w_all(wc, q, 0, 256), 1, 0) + bias_at(biases, 2, x * 512 + q * 256, 256)
            q2[j, :, q * 256 : q * 256 + 256] = (r * (scale * LOG2E)).astype(BF)
        attend(j, q2, k2, v2, a2, lse2, False, hooks)
        project_out(j, a2, wc, 256)
        exchange(1, j)

    cross(0, {1: ("ze1",), 12: ("ze2",)})
    cross(1, {1: ("zs0",), 6: ("ye-1", "ye0", "ye1",), 12: ("zs1",)})

    root_half = 0.7071067811865476
    norm_pdf = 0.3989422804014327

    def hidden_units(j):
        arrived(1, j)
        norm_forward(j, 1, res, biases[4:5, :], gains[1:2, :], biases[7:8, :], n2, r2, x2r)
        for q in range(2):
            def body(i, carry):
                lanes = pl.ds(pl.multiple_of(i * 256, 256), 256)
                h = dot(x2r[j], we[q, :, :, :, lanes].reshape(1024, 256), 1, 0)
                h = h + expb[0:1, pl.ds(pl.multiple_of(x * 2048 + q * 1024 + i * 256, 256), 256)]
                cdf = 0.5 * (1.0 + lax.erf(h * root_half))
                gg[q, j, :, lanes] = (h * cdf).astype(BF)
                gp[q, j, :, lanes] = (cdf + h * (jnp.exp(-0.5 * h * h) * norm_pdf)).astype(BF)
                return carry

            lax.fori_loop(0, 4, body, 0)

    def over_columns(body):
        def step(dn, carry):
            body(dn, pl.ds(pl.multiple_of(dn * 256, 256), 256))
            return carry

        lax.fori_loop(0, 4, step, 0)

    def rows_at(buf, q, dn, lo, hi):
        return buf[q, pl.ds(dn * nq, nq), :, :, lo:hi].reshape(256, hi - lo)

    def units_out(j, src, buf):
        def body(dn, cols):
            acc = dot(src[0, j], rows_at(buf, 0, dn, 0, 1024), 1, 1)
            acc = acc + dot(src[1, j], rows_at(buf, 1, dn, 0, 1024), 1, 1)
            sx[j, :, cols] = acc.astype(BF)

        over_columns(body)

    run("ye2")
    c_event("e")
    hidden_units(0)
    run("zs2", "ys-1", "ys0")
    hidden_units(1)
    run("ys1", "ys2")
    c_event("s")
    units_out(0, gg, ws)
    exchange(2, 0)
    units_out(1, gg, ws)
    exchange(2, 1)
    l_c.wait()
    xs[2].wait_recv()

    def last_norm(j):
        arrived(2, j)
        gain, shift, bias = gains[2:3, :], biases[8:9, :], biases[5:6, :]

        def body(i, carry):
            sa, sb, sc = carry
            rws = pl.ds(pl.multiple_of(i * TILE, TILE), TILE)
            v = res[j, rws, :] + sx[j, rws, :].astype(F32) + rx[0, j, rws, :].astype(F32) + bias
            cen = v - jnp.mean(v, axis=1, keepdims=True)
            r = lax.rsqrt(jnp.mean(cen * cen, axis=1, keepdims=True) + EPS)
            n = cen * r
            xt[rws, :] = (n * gain + shift).astype(BF)
            dz = ct[j, rws, :].astype(F32)
            dt = back_tile(dz, n, r, gain)
            res[j, rws, :] = dt
            ct[j, rws, :] = dt.astype(BF)
            return sa + fold(dz * n), sb + fold(dz), sc + fold(dt)

        zero = jnp.zeros((8, 1024), F32)
        sa, sb, sc = lax.fori_loop(0, rows // TILE, body, (zero, zero, zero))
        add_small(2, sa)
        add_small(11, sb)
        add_small(8, sc)

        @pl.when(x == j)
        def _():
            local(xt, block_out).wait()

    def units_back(j):
        for q in range(2):
            def body(i, carry):
                lanes = pl.ds(pl.multiple_of(i * 256, 256), 256)
                g = dot(ct[j], ws[q, :, :, :, lanes].reshape(1024, 256), 1, 0)
                g = (g * gp[q, j, :, lanes].astype(F32)).astype(BF)
                gp[q, j, :, lanes] = g
                sm[pl.ds(13 + 2 * x + q, 1), lanes] += jnp.sum(g.astype(F32), axis=0, keepdims=True)
                return carry

            lax.fori_loop(0, 4, body, 0)
        units_out(j, gp, we)
        exchange(3, j)

    last_norm(0)
    units_back(0)
    last_norm(1)
    units_back(1)

    def grad_into(dst, pieces, first=0):
        def body(i, carry):
            lanes = pl.ds(pl.multiple_of(i * 256, 256), 256)
            lo = first
            for left, right in pieces:
                g = dot(left[:, :, lanes].reshape(512, 256), right, 0, 0)
                w = g.shape[1]
                dst[pl.ds(i * nq, nq), :, :, lo : lo + w] = g.astype(BF).reshape(nq, 2, sh, w)
                lo += w
            return carry

        lax.fori_loop(0, 4, body, 0)

    own_of = {0: own.at[0], 1: own.at[1], 2: we.at[0], 3: we.at[1]}
    send_of = {0: ws.at[0], 1: ws.at[1], 2: ws.at[0], 3: ws.at[1]}
    units = [(0, 0, 1024), (1, 0, 1024), (2, 0, 256), (2, 256, 1024)] + [(3, 256 * p, 256 * p + 256) for p in range(4)]
    z_to = {k: lax.rem(z + k, nz) for k in peers_z}
    gsend, gy, gz_ = [], [], []
    for g, lo, hi in units:
        gsend.append(plan(send_of[g].at[:, :, :, lo:hi], cland.at[g, :, :, :, lo:hi], c_dev))
        gy.append(plan(own_of[g].at[:, ny, :, lo:hi], yland.at[g, :, :, lo:hi], y_dev))
        gz_.append([plan(own_of[g].at[z_to[k], y, :, lo:hi], zland.at[g, k, :, lo:hi], z_dev(k)) for k in peers_z])

    def unit_pair(ref, q):
        return ref[q].reshape(512, 1024)

    for g in ("e", "s"):
        for kind in (zc, yc, cz, cy):
            for cp in kind[g].values():
                sent(cp)
    grad_into(send_of[0], [(x2r, unit_pair(gp, nc))])
    launch(gsend[0])
    grad_into(own_of[0], [(x2r, unit_pair(gp, c))])
    grad_into(send_of[1], [(ct, unit_pair(gg, nc))])
    launch(gsend[1])
    grad_into(own_of[1], [(ct, unit_pair(gg, c))])
    l_en2a = local(enc, x2r.at[x])
    l_en2b = local(eland.at[nx], x2r.at[nx])


    def grad_core(u):
        g, lo, hi = units[u]
        gsend[u].wait_recv()
        local(cland.at[g, :, :, :, lo:hi], tmp.at[:, :, :, lo:hi]).wait()
        o = own_of[g]

        def body(i, carry):
            blk = pl.ds(i * nq, nq)
            o[blk, :, :, lo:hi] = (o[blk, :, :, lo:hi].astype(F32) + tmp[blk, :, :, lo:hi].astype(F32)).astype(BF)
            return carry

        lax.fori_loop(0, 4, body, 0)
        launch(gy[u])

    def grad_y(u):
        g, lo, hi = units[u]
        gy[u].wait_recv()
        local(yland.at[g, :, :, lo:hi], tmp.at[:, 0, :, lo:hi]).wait()
        o = own_of[g]

        def body(i, carry):
            blk = pl.ds(i * nq, nq)
            o[blk, y, :, lo:hi] = (o[blk, y, :, lo:hi].astype(F32) + tmp[blk, 0, :, lo:hi].astype(F32)).astype(BF)
            return carry

        lax.fori_loop(0, 4, body, 0)
        for cp in gz_[u]:
            launch(cp)

    def grad_z(u, out):
        g, lo, hi = units[u]
        cps = []
        for k in peers_z:
            gz_[u][k - 1].wait_recv()
            cps.append(local(zland.at[g, k, :, lo:hi], tmp.at[k, 0, :, lo:hi]))
        for cp in cps:
            cp.wait()
        acc = own_of[g][z, y, :, lo:hi].astype(F32)
        for k in peers_z:
            acc = acc + tmp[k, 0, :, lo:hi].astype(F32)
        outf[:, lo:hi] = acc
        local(outf.at[:, lo:hi], out.at[:, lo:hi]).wait()

    def sum_rows(row, src, col):
        sm[row : row + 1, pl.ds(pl.multiple_of(col, 256), 256)] += jnp.sum(src.astype(F32), axis=0, keepdims=True)

    def heads_back(j, buf, lo, q_ref, k_ref, v_ref, o_ref, l_ref, causal, hooks):
        for q in range(2):
            do[:, q * 256 : q * 256 + 256] = dot(ct[j], w_all(buf, q, lo, lo + 256), 1, 0).astype(BF)
        attend_back(j, q_ref, k_ref, v_ref, o_ref, l_ref, causal, hooks)

    def swap_kv(slot):
        for j in range(2):
            ksend[0, j] = dk[2 * j + nc].astype(BF)
            ksend[1, j] = dv[2 * j + nc].astype(BF)
        return send(ksend, krecv.at[slot], c_dev)

    def join_kv(slot):
        for j in range(2):
            krecv[slot, 0, j] = (dk[2 * j + c] + krecv[slot, 0, j].astype(F32)).astype(BF)
            krecv[slot, 1, j] = (dv[2 * j + c] + krecv[slot, 1, j].astype(F32)).astype(BF)

    def head_cols(ref, q):
        return ref[:, :, pl.ds(pl.multiple_of(q * 256, 256), 256)].reshape(512, 256)

    def cross_back(j, hooks):
        arrived(3, j)
        norm_back(j, 3, gains[1:2, :], n2, r2, 1, 10, 7)
        if j == 1:
            sent(gsend[0])
            grad_into(send_of[2], [(ct, head_cols(a2, nc))])
            launch(gsend[2])
            grad_into(own_of[2], [(ct, head_cols(a2, c))])
        heads_back(j, wc, 256, q2, k2, v2, a2, lse2, False, hooks)
        for dn in range(4):
            acc = dot(dq[j, :, 0:256], w_rows(wc, 0, dn, 0, 256), 1, 1)
            acc = acc + dot(dq[j, :, 256:512], w_rows(wc, 1, dn, 0, 256), 1, 1)
            sx[j, :, dn * 256 : dn * 256 + 256] = acc.astype(BF)
        exchange(4, j)

    part = functools.partial
    grad_core(0)
    cross_back(0, ({}, {2: part(grad_core, 1)}))
    cross_back(1, ({6: part(grad_y, 0)}, {4: part(grad_core, 2)}))
    swap2 = swap_kv(0)
    for j in range(2):
        for q in range(2):
            sum_rows(5, dq[j, :, q * 256 : q * 256 + 256], x * 512 + q * 256)
    swap2.wait_recv()
    join_kv(0)
    for j in range(2):
        for q in range(2):
            sum_rows(6, krecv[0, 1, j, :, q * 256 : q * 256 + 256], x * 512 + q * 256)
    l_en2a.wait()
    l_en2b.wait()

    def cross_pieces(q):
        return [
            (x1r, head_cols(dq, q)),
            (x2r, head_cols(krecv.at[0, 0], q)),
            (x2r, head_cols(krecv.at[0, 1], q)),
        ]

    grad_into(send_of[2], cross_pieces(nc), 256)
    launch(gsend[3])
    grad_into(own_of[2], cross_pieces(c), 256)
    l_x2a = local(hid, x1r.at[x])
    l_x2b = local(xland.at[nx], x1r.at[nx])

    def input_part(j, terms, dn):
        acc = None
        for ref, buf, lo in terms:
            for q in range(2):
                part = dot(ref[j, :, q * 256 : q * 256 + 256], rows_at(buf, q, dn, lo, lo + 256), 1, 1)
                acc = part if acc is None else acc + part
        return acc

    enc_terms = [(krecv.at[0, 0], wb, 256), (krecv.at[0, 1], wb, 512)]
    def part_of_enc_terms_xt(dn, cols):
        xt[:, cols] = input_part(nx, enc_terms, dn).astype(BF)

    over_columns(part_of_enc_terms_xt)
    def part_of_enc_terms_den(dn, cols):
        den[:, cols] = input_part(x, enc_terms, dn)

    over_columns(part_of_enc_terms_den)
    enc_x = send(xt, rxd.at[0], x_dev)

    def self_back(j, hooks):
        arrived(4, j)
        norm_back(j, 4, gains[0:1, :], n1, r1, 0, 9, 12)
        if j == 1:
            sent(gsend[1])
            grad_into(send_of[3], [(ct, head_cols(ao, nc))])
            launch(gsend[4])
            grad_into(own_of[3], [(ct, head_cols(ao, c))])
        heads_back(j, wb, 0, qs, ks, vs, ao, lse1, True, hooks)

    self_back(0, ({1: part(grad_core, 3), 6: part(grad_y, 1)}, {6: part(grad_y, 2)}))
    sent(enc_x)
    self_back(1, ({5: part(grad_core, 4)}, {2: part(grad_z, 0, ge_out)}))
    sent(swap2)
    swap1 = swap_kv(1)
    l_x2a.wait()
    l_x2b.wait()
    grad_into(send_of[3], [(x1r, head_cols(dq, nc))], 256)
    launch(gsend[5])
    grad_into(own_of[3], [(x1r, head_cols(dq, c))], 256)
    for j in range(2):
        for q in range(2):
            sum_rows(3, dq[j, :, q * 256 : q * 256 + 256], x * 512 + q * 256)
    swap1.wait_recv()
    join_kv(1)
    grad_into(send_of[3], [(x1r, head_cols(krecv.at[1, i], nc)) for i in range(2)], 512)
    launch(gsend[6])
    launch(gsend[7])
    grad_core(5)
    grad_y(3)
    in_terms = [(dq, wa, 0), (krecv.at[1, 0], wa, 256), (krecv.at[1, 1], wa, 512)]
    def part_of_in_terms_xt(dn, cols):
        xt[:, cols] = input_part(nx, in_terms, dn).astype(BF)

    over_columns(part_of_in_terms_xt)
    hid_x = send(xt, rxd.at[1], x_dev)
    grad_into(own_of[3], [(x1r, head_cols(krecv.at[1, i], c)) for i in range(2)], 512)
    grad_core(6)
    grad_core(7)
    for j in range(2):
        for q in range(2):
            sum_rows(4, krecv[1, 1, j, :, q * 256 : q * 256 + 256], x * 512 + q * 256)
    s1 = send(sm, smr.at[0], c_dev)
    grad_y(4)
    def part_of_in_terms_res(dn, cols):
        res[x, :, cols] += input_part(x, in_terms, dn)

    over_columns(part_of_in_terms_res)
    s1.wait_recv()
    sent(s1)
    sm[...] += smr[0]
    s2 = send(sm, smr.at[1], x_dev)
    sent(hid_x)
    enc_x.wait_recv()
    den[...] += rxd[0].astype(F32)
    o1 = local(den, enc_out)
    grad_y(5)
    s2.wait_recv()
    sent(s2)
    sm[...] += smr[1]
    s3 = send(sm, smr.at[2], y_dev)
    grad_z(1, gs_out)
    hid_x.wait_recv()
    res[x] += rxd[1].astype(F32)
    o2 = local(res.at[x], hid_out)
    grad_y(6)
    s3.wait_recv()
    sent(s3)
    sm[...] += smr[2]
    smz[z] = sm[...]
    s4 = [send(sm, smz.at[z], z_dev(k)) for k in range(1, nz)]
    grad_y(7)
    grad_z(2, gc_out)
    grad_z(3, gc_out)
    grad_z(4, ga_out)
    grad_z(5, ga_out)
    for cp in s4:
        cp.wait_recv()
        sent(cp)
    acc = smz[0]
    for k in range(1, nz):
        acc = acc + smz[k]
    sm[...] = acc
    o3 = local(sm, small_out)
    grad_z(6, ga_out)
    grad_z(7, ga_out)
    for cp in (o1, o2, o3):
        cp.wait()
    for cp in list(pending):
        sent(cp)


def run_layer(nz, sh, prefix, hid, enc, cot, shards, gains, biases, selfb, expb):
    any_spec = pl.BlockSpec(memory_space=pl.ANY)
    vmem = pl.BlockSpec(memory_space=pltpu.VMEM)
    rows = hid.shape[0]
    shape = jax.ShapeDtypeStruct
    outs = [
        shape((rows, 1024), BF),
        shape((rows, 1024), F32),
        shape((rows, 1024), F32),
        shape((sh, 1024), F32),
        shape((sh, 1024), F32),
        shape((sh, 1024), F32),
        shape((sh, 1024), F32),
        shape((SMALL_ROWS, 1024), F32),
        shape((2, rows, 1024), BF),
        shape((2, rows, 1024), BF),
        shape((4, nz, 2, sh, 1024), BF),
        shape((4, nz, sh, 1024), BF),
        shape((4, nz, sh, 1024), BF),
    ]

    def weight(n):
        return pltpu.VMEM((2, nz, 2, sh, n), BF)

    def acts(n, kind=BF):
        return pltpu.VMEM((2, rows, n), kind)

    def keys(kind=BF):
        return pltpu.VMEM((4, rows, 512), kind)

    scratch = [
        weight(768),
        weight(768),
        weight(512),
        weight(1024),
        weight(1024),
        acts(1024),
        acts(1024),
        acts(1024),
        acts(512),
        keys(),
        keys(),
        acts(512),
        acts(512),
        keys(),
        keys(),
        acts(512),
        pltpu.VMEM((2, 2, rows, 1024), BF),
        pltpu.VMEM((2, 2, rows, 1024), BF),
        acts(1024),
        acts(1024),
        acts(128, F32),
        acts(128, F32),
        acts(128, F32),
        acts(128, F32),
        acts(1024, F32),
        acts(1024),
        pltpu.VMEM((2, 2, rows, 1024), BF),
        acts(1024),
        acts(512),
        pltpu.VMEM((rows, 512), BF),
        keys(F32),
        keys(F32),
        pltpu.VMEM((2, 2, rows, 512), BF),
        pltpu.VMEM((2, 2, 2, rows, 512), BF),
        pltpu.VMEM((2, 1024, 1024), BF),
        pltpu.VMEM((2, nz, 2, sh, 1024), BF),
        pltpu.VMEM((nz, 2, sh, 1024), BF),
        pltpu.VMEM((rows, 1024), BF),
        pltpu.VMEM((1024, 256), BF),
        pltpu.VMEM((1024, 256), BF),
        pltpu.VMEM((rows, 1024), F32),
        pltpu.VMEM((sh, 1024), F32),
        pltpu.VMEM((SMALL_ROWS, 1024), F32),
        pltpu.VMEM((3, SMALL_ROWS, 1024), F32),
        pltpu.VMEM((nz, SMALL_ROWS, 1024), F32),
        pltpu.SemaphoreType.DMA((200 + 60 * nz,)),
    ]
    return pl.pallas_call(
        functools.partial(layer_kernel, nz, sh),
        out_shape=outs,
        in_specs=[pl.BlockSpec(memory_space=pltpu.SMEM)] + [any_spec] * 8 + [vmem] * 4,
        out_specs=[any_spec] * len(outs),
        scratch_shapes=scratch,
        compiler_params=pltpu.CompilerParams(
            collective_id=0, has_side_effects=True, vmem_limit_bytes=67043328
        ),
    )(prefix, hid, enc, cot, *shards, gains, biases, selfb, expb)


def per_device(
    hidden,
    encoder,
    prefix,
    query_self,
    key_self,
    value_self,
    output_self,
    cross_query_matrix,
    key_cross,
    value_cross,
    output_cross,
    expand,
    shrink,
    norm_gains,
    biases,
    self_out_bias,
    expand_bias,
    cotangent,
):
    sh = query_self.shape[1]
    nz = 1024 // sh // 2
    shards = (
        jnp.concatenate([query_self[0], key_self[0], value_self[0]], axis=1),
        jnp.concatenate([output_self[0].T, key_cross[0], value_cross[0]], axis=1),
        jnp.concatenate([cross_query_matrix[0], output_cross[0].T], axis=1),
        expand[0],
        shrink[0].T,
    )
    outs = run_layer(
        nz,
        sh,
        prefix,
        hidden[0],
        encoder[0],
        cotangent[0],
        shards,
        norm_gains[0],
        biases[0],
        self_out_bias,
        expand_bias,
    )
    block, grad_hid, grad_enc, ge, gs, gc, ga, small = outs[:8]

    def part(g, i):
        return g[:, i * 256 : i * 256 + 256]

    return (
        block[None],
        grad_hid[None],
        grad_enc[None],
        part(ga, 1)[None],
        part(ga, 2)[None],
        part(ga, 3)[None],
        part(ga, 0).T[None],
        part(gc, 1)[None],
        part(gc, 2)[None],
        part(gc, 3)[None],
        part(gc, 0).T[None],
        ge[None],
        gs.T[None],
        small[0:3][None],
        small[3:12][None],
        small[12:13],
        small[13:17].reshape(1, 4096),
    )


def solution(mesh):
    in_specs = (
        P("dp", "tensor", None),
        P("dp", "tensor", None),
        P("dp"),
        P(None, "dp", "tensor"),
        P(None, "dp", "tensor"),
        P(None, "dp", "tensor"),
        P(None, "tensor", "dp"),
        P(None, "dp", "tensor"),
        P(None, "dp", "tensor"),
        P(None, "dp", "tensor"),
        P(None, "tensor", "dp"),
        P(None, "dp", "tensor"),
        P(None, "tensor", "dp"),
        P(),
        P(),
        P(),
        P(),
        P("dp", "tensor", None),
    )
    out_specs = (
        P("dp", "tensor", None),
        P("dp", "tensor", None),
        P("dp", "tensor", None),
        P(None, "dp", "tensor"),
        P(None, "dp", "tensor"),
        P(None, "dp", "tensor"),
        P(None, "tensor", "dp"),
        P(None, "dp", "tensor"),
        P(None, "dp", "tensor"),
        P(None, "dp", "tensor"),
        P(None, "tensor", "dp"),
        P(None, "dp", "tensor"),
        P(None, "tensor", "dp"),
        P(),
        P(),
        P(),
        P(),
    )
    return jax.shard_map(
        per_device, mesh=mesh, in_specs=in_specs, out_specs=out_specs, check_vma=False
    )
```

```python
import functools

import jax
import jax.numpy as jnp
from jax import lax
from jax.experimental import pallas as pl
from jax.experimental.pallas import tpu as pltpu
from jax.sharding import PartitionSpec as P

MESH = pl.DeviceIdType.MESH
BF = jnp.bfloat16
F32 = jnp.float32
EPS = 1e-05
HEAD = 64
LOG2E = 1.4426950408889634
LN2 = 0.6931471805599453
NEG = -1e30
SMALL_ROWS = 24


def dot(a, b, ca, cb):
    return lax.dot_general(a, b, (((ca,), (cb,)), ((), ())), preferred_element_type=F32)


def layer_kernel(nz, sh, *refs):
    (
        prefix,
        hid,
        enc,
        cot,
        q_in,
        k_in,
        v_in,
        o_in,
        k2_in,
        v2_in,
        q2_in,
        o2_in,
        we_in,
        ws_in,
        gains,
        biases,
        selfb,
        expb,
        block_out,
        hid_out,
        enc_out,
        ge_out,
        gs_out,
        gc_out,
        ga_out,
        gain_out,
        bias_out,
        selfb_out,
        expb_out,
        xland,
        eland,
        cland,
        yland,
        zland,
        wa,
        wb,
        wc,
        we,
        ws,
        x1r,
        x2r,
        ct,
        qs,
        ks,
        vs,
        ao,
        q2,
        k2,
        v2,
        a2,
        gg,
        gp,
        n1,
        n2,
        r1,
        r2,
        lse1,
        lse2,
        res,
        sx,
        rx,
        rxd,
        dq,
        do,
        dk,
        dv,
        ksend,
        krecv,
        cs,
        own,
        tmp,
        xt,
        dom,
        qm,
        den,
        outf,
        sm,
        smr,
        smz,
        sems,
    ) = refs
    d = lax.axis_index("dp")
    t = lax.axis_index("tensor")
    x, c = t // 2, t % 2
    z, y = d // 2, d % 2
    nx, nc, ny = 1 - x, 1 - c, 1 - y
    x_dev = (d, nx * 2 + c)
    c_dev = (d, x * 2 + nc)
    y_dev = (z * 2 + ny, t)

    def z_dev(k):
        return (lax.rem(z + k, nz) * 2 + y, t)

    def z_from(k):
        return lax.rem(z + nz - k, nz)

    nq = nz // 4
    rows = hid.shape[0]
    count = [0]

    def new_sem():
        count[0] += 1
        return sems.at[count[0] - 1]

    pending = []

    def plan(src, dst, dev):
        return pltpu.make_async_remote_copy(
            src_ref=src, dst_ref=dst, send_sem=new_sem(), recv_sem=new_sem(), device_id=dev, device_id_type=MESH
        )

    def launch(cp):
        cp.start()
        pending.append(cp)
        return cp

    def send(src, dst, dev):
        return launch(plan(src, dst, dev))

    def sent(cp):
        cp.wait_send()
        pending[:] = [other for other in pending if other is not cp]

    def local(src, dst):
        cp = pltpu.make_async_copy(src, dst, new_sem())
        cp.start()
        return cp

    barrier = pltpu.get_barrier_semaphore()
    peers = [x_dev, c_dev, y_dev] + [z_dev(k) for k in range(1, nz)]
    for dev in peers:
        pl.semaphore_signal(barrier, inc=1, device_id=dev, device_id_type=MESH)
    pl.semaphore_wait(barrier, len(peers))

    xs = [send(hid, xland.at[x], x_dev)]
    groups = {
        "a": ([q_in, k_in, v_in], wa),
        "b": ([o_in, k2_in, v2_in], wb),
        "c": ([q2_in, o2_in], wc),
        "e": ([we_in], we),
        "s": ([ws_in], ws),
    }

    class Bundle:
        def __init__(self, copies):
            self.copies = copies

        def start(self):
            for cp in self.copies:
                cp.start()

        def wait_recv(self):
            for cp in self.copies:
                cp.wait_recv()

        def wait_send(self):
            for cp in self.copies:
                cp.wait_send()

        def wait(self):
            for cp in self.copies:
                cp.wait()

    def columns_of(srcs, g, spot):
        width = srcs[0].shape[1]
        buf = groups[g][1]
        for i, src in enumerate(srcs):
            yield src, buf.at[(*spot, slice(None), slice(i * width, i * width + width))]

    def plan_own(g, dev):
        return Bundle([plan(src, dst, dev) for src, dst in columns_of(groups[g][0], g, (c, z, y))])

    zc, yc, cz, cy, lc = {}, {}, {}, {}, {}
    peers_z = range(1, nz)

    for g in groups:
        buf = groups[g][1]
        zc[g] = {k: plan_own(g, z_dev(k)) for k in peers_z}
        yc[g] = {0: plan_own(g, y_dev)}
        cz[g] = {0: plan_own(g, c_dev)}
        cy[g] = {}
        for k in range(nz):
            zk = z_from(k)
            if k:
                spot = buf.at[c, zk, y]
                yc[g][k] = plan(spot, spot, y_dev)
                cz[g][k] = plan(spot, spot, c_dev)
            spot = buf.at[c, zk, ny]
            cy[g][k] = plan(spot, spot, c_dev)

    def start_z(g):
        for k in peers_z:
            launch(zc[g][k])

    def start_y(g):
        launch(yc[g][0])

    def start_c(g):
        launch(cz[g][0])
        lc[g] = Bundle([local(src, dst) for src, dst in columns_of(groups[g][0], g, (c, z, y))])

    def thirds(part):
        return range(1 + (nz - 1) * part // 3, 1 + (nz - 1) * (part + 1) // 3)

    def z_event(g, part):
        for k in thirds(part):
            zc[g][k].wait_recv()
            launch(yc[g][k])
            launch(cz[g][k])

    def y_event(g, part):
        for k in [0] if part < 0 else thirds(part):
            yc[g][k].wait_recv()
            launch(cy[g][k])

    def c_event(g):
        lc[g].wait()
        for cp in list(cz[g].values()) + list(cy[g].values()):
            cp.wait_recv()

    def run(*words):
        for word in words:
            kind, g, part = word[0], word[1], int(word[2:] or 0)
            if kind == "o":
                start_y(g)
            else:
                (z_event if kind == "z" else y_event)(g, part)

    start_z("a")
    start_y("a")
    start_c("a")
    l_x = local(hid, x1r.at[x])
    l_e = local(enc, x2r.at[x])
    l_c = local(cot, ct.at[x])
    start_z("b")
    start_y("b")
    start_c("b")
    xs.append(send(enc, eland.at[x], x_dev))
    xs.append(send(cot, ct.at[x], x_dev))
    for g in ("c", "e", "s"):
        start_z(g)
        start_c(g)

    def hooked(hooks, i):
        for at, text in hooks.items():
            if isinstance(text, tuple):
                pl.when(i == at // 2 * 2)(functools.partial(run, *text))
            else:
                pl.when(i == at // 2 * 2)(text)

    def w_all(buf, q, lo, hi):
        return buf[q, :, :, :, lo:hi].reshape(1024, hi - lo)

    def bias_at(ref, row, lo, width):
        return ref[row, :, pl.ds(pl.multiple_of(lo, 256), width)]

    sm[...] = jnp.zeros_like(sm)

    def fold(v):
        return jnp.sum(v.reshape(v.shape[0] // 8, 8, v.shape[1]), axis=0)

    scale = HEAD**-0.5

    l_x.wait()
    xs[0].wait_recv()
    l_xn = local(xland.at[nx], x1r.at[nx])
    run("za0", "ya-1", "za1", "ya0", "za2", "oc", "ya1", "ya2")
    l_xn.wait()
    c_event("a")
    kv1 = []
    for j in range(2):
        xj = x1r[j]
        for q in range(2):
            r = dot(xj, w_all(wa, q, 0, 768), 1, 0)
            lanes = slice(q * 256, q * 256 + 256)
            col = x * 512 + q * 256
            qs[j, :, lanes] = ((r[:, :256] + bias_at(biases, 0, col, 256)) * (scale * LOG2E)).astype(BF)
            ks[2 * j + c, :, lanes] = r[:, 256:512].astype(BF)
            vs[2 * j + c, :, lanes] = (r[:, 512:] + bias_at(biases, 1, col, 256)).astype(BF)
        kv1 += [send(b.at[2 * j + c], b.at[2 * j + c], c_dev) for b in (ks, vs)]
        run(*(("zb0", "oe") if j == 0 else ("zb1",)))
    xs[1].wait_recv()
    l_en = local(eland.at[nx], x2r.at[nx])

    lane256 = lax.broadcasted_iota(jnp.int32, (128, 256), 1)
    lane128 = lax.broadcasted_iota(jnp.int32, (128, 128), 1)
    zero_bf = jnp.zeros((128, 256), BF)
    lane256w = lax.broadcasted_iota(jnp.int32, (256, 256), 1)
    lane128w = lax.broadcasted_iota(jnp.int32, (256, 128), 1)
    zero_bfw = jnp.zeros((256, 256), BF)
    limit = prefix[0]

    def parts_of(keys, causal, j):
        if not causal:
            return [(0, 4, False)]
        return [(0, 2, True)] if j == 0 else [(0, 2, False), (2, 4, True)]

    def scores(qh, k_ref, part, lanes, j, row0):
        b0, b1, masked = part
        k = k_ref[b0:b1, :, lanes].reshape((b1 - b0) * 256, 256)
        s = dot(qh, k, 1, 1)
        if masked:
            cols = b0 * 256 + lax.broadcasted_iota(jnp.int32, s.shape, 1)
            rws = (2 * j + c) * 256 + row0 + lax.broadcasted_iota(jnp.int32, s.shape, 0)
            s = jnp.where((cols <= rws) | (cols < limit), s, NEG)
        return s

    def attend(j, q_ref, k_ref, v_ref, o_ref, l_ref, causal, hooks):
        parts = parts_of(k_ref, causal, j)

        def body(i, carry):
            hooked(hooks, 2 * i)
            h = i
            row0 = 0
            rws = slice(0, 256)
            lanes = pl.ds(pl.multiple_of((h // 4) * 256, 256), 256)
            head = (lane256w // HEAD) == (h % 4)
            qh = jnp.where(head, q_ref[j, rws, lanes], zero_bfw)
            ss = [scores(qh, k_ref, p, lanes, j, row0) for p in parts]
            m = functools.reduce(jnp.maximum, [jnp.max(s, axis=1, keepdims=True) for s in ss])
            total = jnp.zeros((256, 1), F32)
            o = jnp.zeros((256, 256), F32)
            for s, (b0, b1, _) in zip(ss, parts):
                p = jnp.exp2(s - m)
                total = total + jnp.sum(p, axis=1, keepdims=True)
                o = o + dot(p.astype(BF), v_ref[b0:b1, :, lanes].reshape((b1 - b0) * 256, 256), 1, 0)
            o = o / total
            o_ref[j, rws, lanes] = jnp.where(head, o.astype(BF), o_ref[j, rws, lanes])
            l_ref[j, rws, :] = jnp.where(lane128w == h, m + jnp.log2(total), l_ref[j, rws, :])
            return carry

        lax.fori_loop(0, 8, body, 0)

    def attend_back(j, q_ref, k_ref, v_ref, o_ref, l_ref, causal, hooks):
        parts = parts_of(k_ref, causal, j)
        nk = 256 * parts[-1][1]
        for qt in range(2):
            lanes = slice(qt * 256, qt * 256 + 256)

            def body(i, carry):
                hooked(hooks[qt], 2 * i)
                h = i
                row0 = 0
                rws = slice(0, 256)
                spot = pl.ds(pl.multiple_of(i * 256, 256), 256)
                head = (lane256w // HEAD) == h
                qh = jnp.where(head, q_ref[j, rws, lanes], zero_bfw)
                dh = jnp.where(head, do[rws, lanes], zero_bfw)
                delta = jnp.sum(dh.astype(F32) * o_ref[j, rws, lanes].astype(F32), axis=1, keepdims=True)
                lse = jnp.sum(jnp.where(lane128w == h + 4 * qt, l_ref[j, rws, :], 0.0), axis=1, keepdims=True)
                g = jnp.zeros((256, 256), F32)
                for part in parts:
                    b0, b1, _ = part
                    s = scores(qh, k_ref, part, lanes, j, row0)
                    p = jnp.exp2(s - lse)
                    dp = dot(dh, v_ref[b0:b1, :, lanes].reshape((b1 - b0) * 256, 256), 1, 1)
                    ds = (p * (dp - delta)).astype(BF)
                    cs[0, spot, b0 * 256 : b1 * 256] = p.astype(BF)
                    cs[1, spot, b0 * 256 : b1 * 256] = ds
                    g = g + dot(ds, k_ref[b0:b1, :, lanes].reshape((b1 - b0) * 256, 256), 1, 0)
                dq[j, rws, lanes] = jnp.where(head, (g.astype(BF) * scale).astype(BF), dq[j, rws, lanes])
                dom[spot, :] = dh
                qm[spot, :] = qh
                return carry

            lax.fori_loop(0, 4, body, 0)
            for b in range(nk // 256):
                keys = slice(b * 256, b * 256 + 256)
                gv = dot(cs[0, :, keys], dom[...], 0, 0)
                gk = dot(cs[1, :, keys], qm[...], 0, 0) * LN2
                if j == 0:
                    dv[b, :, lanes] = gv
                    dk[b, :, lanes] = gk
                else:
                    dv[b, :, lanes] += gv
                    dk[b, :, lanes] += gk
        if j == 0 and nk < 1024:
            dv[2:4] = jnp.zeros((2, 256, 512), F32)
            dk[2:4] = jnp.zeros((2, 256, 512), F32)

    def over_columns(body):
        def step(dn, carry):
            body(dn, pl.ds(pl.multiple_of(dn * 256, 256), 256))
            return carry

        lax.fori_loop(0, 4, step, 0)

    def rows_at(buf, q, dn, lo, hi):
        return buf[q, pl.ds(dn * nq, nq), :, :, lo:hi].reshape(256, hi - lo)

    def project_out(j, src, buf, lo):
        def body(dn, cols):
            acc = dot(src[j, :, 0:256], rows_at(buf, 0, dn, lo, lo + 256), 1, 1)
            acc = acc + dot(src[j, :, 256:512], rows_at(buf, 1, dn, lo, lo + 256), 1, 1)
            sx[j, :, cols] = acc.astype(BF)

        over_columns(body)

    ex = {}

    def exchange(stage, j):
        ex[stage, j] = send(sx.at[j], rx.at[stage % 2, j], x_dev)

    def arrived(stage, j):
        ex[stage, j].wait_recv()
        sent(ex[stage, j])

    TILE = 32

    def norm_forward(j, stage, base, bias, gain, shift, n_ref, r_ref, low_ref):
        def body(i, carry):
            rws = pl.ds(pl.multiple_of(i * TILE, TILE), TILE)
            v = base[j, rws, :].astype(F32) + sx[j, rws, :].astype(F32) + rx[stage % 2, j, rws, :].astype(F32) + bias
            cen = v - jnp.mean(v, axis=1, keepdims=True)
            r = lax.rsqrt(jnp.mean(cen * cen, axis=1, keepdims=True) + EPS)
            n = cen * r
            o = n * gain + shift
            n_ref[j, rws, :] = n.astype(BF)
            r_ref[j, rws, :] = jnp.broadcast_to(r, (TILE, 128))
            res[j, rws, :] = o
            low_ref[j, rws, :] = o.astype(BF)
            return carry

        lax.fori_loop(0, rows // TILE, body, 0)

    def add_small(row, v):
        sm[row : row + 1, :] += jnp.sum(v, axis=0, keepdims=True) * 0.5

    def back_tile(dz, n, r, gain):
        gz = gain * dz
        ma = jnp.mean(gz, axis=1, keepdims=True)
        mb = jnp.mean(gz * n, axis=1, keepdims=True)
        return (gz - ma - n * mb) * r

    def norm_back(j, stage, gain, n_ref, r_ref, gain_row, shift_row, bias_row):
        def body(i, carry):
            sa, sb, sc = carry
            rws = pl.ds(pl.multiple_of(i * TILE, TILE), TILE)
            dz = res[j, rws, :] + sx[j, rws, :].astype(F32) + rx[stage % 2, j, rws, :].astype(F32)
            n = n_ref[j, rws, :].astype(F32)
            dt = back_tile(dz, n, r_ref[j, rws, 0:1], gain)
            res[j, rws, :] = dt
            ct[j, rws, :] = dt.astype(BF)
            return sa + fold(dz * n), sb + fold(dz), sc + fold(dt)

        zero = jnp.zeros((8, 1024), F32)
        sa, sb, sc = lax.fori_loop(0, rows // TILE, body, (zero, zero, zero))
        add_small(gain_row, sa)
        add_small(shift_row, sb)
        add_small(bias_row, sc)

    for cp in kv1:
        cp.wait_recv()
    attend(0, qs, ks, vs, ao, lse1, True, {5: ("zb2",), 14: ("zc0", "os",)})
    run("yb-1", "yb0", "yb1", "zc1", "yb2")
    c_event("b")
    project_out(0, ao, wb, 0)
    exchange(0, 0)
    attend(1, qs, ks, vs, ao, lse1, True, {4: ("zc2",), 13: ("yc-1", "yc0",)})
    project_out(1, ao, wb, 0)
    exchange(0, 1)
    run("ze0", "yc1", "yc2")
    l_e.wait()
    l_en.wait()
    def encoder_part(i, carry):
        j, q = i // 2, i % 2
        r = dot(x2r[j], w_all(wb, q, 256, 768), 1, 0)
        lanes = pl.ds(pl.multiple_of(q * 256, 256), 256)
        k2[2 * j + c, :, lanes] = r[:, :256].astype(BF)
        v2[2 * j + c, :, lanes] = (r[:, 256:] + bias_at(biases, 3, x * 512 + q * 256, 256)).astype(BF)
        return carry

    lax.fori_loop(0, 4, encoder_part, 0)
    kv2 = [send(b.at[2 * j + c], b.at[2 * j + c], c_dev) for j in range(2) for b in (k2, v2)]
    c_event("c")
    for cp in kv2:
        cp.wait_recv()

    def cross(j, hooks):
        arrived(0, j)
        norm_forward(j, 0, x1r, selfb[0:1, :], gains[0], biases[6], n1, r1, x1r)

        def body(q, carry):
            r = dot(x1r[j], w_all(wc, q, 0, 256), 1, 0) + bias_at(biases, 2, x * 512 + q * 256, 256)
            q2[j, :, pl.ds(pl.multiple_of(q * 256, 256), 256)] = (r * (scale * LOG2E)).astype(BF)
            return carry

        lax.fori_loop(0, 2, body, 0)
        attend(j, q2, k2, v2, a2, lse2, False, hooks)
        project_out(j, a2, wc, 256)
        exchange(1, j)

    cross(0, {1: ("ze1",), 12: ("ze2",)})
    cross(1, {1: ("zs0",), 6: ("ye-1", "ye0", "ye1",), 12: ("zs1",)})

    root_half = 0.7071067811865476
    norm_pdf = 0.3989422804014327

    def hidden_units(j):
        arrived(1, j)
        norm_forward(j, 1, res, biases[4], gains[1], biases[7], n2, r2, x2r)

        def body(step, carry):
            q, i = step // 4, step % 4
            lanes = pl.ds(pl.multiple_of(i * 256, 256), 256)
            h = dot(x2r[j], we[q, :, :, :, lanes].reshape(1024, 256), 1, 0)
            h = h + expb[0:1, pl.ds(pl.multiple_of(x * 2048 + step * 256, 256), 256)]
            cdf = 0.5 * (1.0 + lax.erf(h * root_half))
            gg[q, j, :, lanes] = (h * cdf).astype(BF)
            gp[q, j, :, lanes] = (cdf + h * (jnp.exp(-0.5 * h * h) * norm_pdf)).astype(BF)
            return carry

        lax.fori_loop(0, 8, body, 0)

    def units_out(j, src, buf):
        def body(dn, cols):
            acc = dot(src[0, j], rows_at(buf, 0, dn, 0, 1024), 1, 1)
            acc = acc + dot(src[1, j], rows_at(buf, 1, dn, 0, 1024), 1, 1)
            sx[j, :, cols] = acc.astype(BF)

        over_columns(body)

    run("ye2")
    c_event("e")
    hidden_units(0)
    run("zs2", "ys-1", "ys0")
    hidden_units(1)
    run("ys1", "ys2")
    c_event("s")
    units_out(0, gg, ws)
    exchange(2, 0)
    units_out(1, gg, ws)
    exchange(2, 1)
    l_c.wait()
    xs[2].wait_recv()

    def last_norm(j):
        arrived(2, j)
        gain, shift, bias = gains[2], biases[8], biases[5]

        def body(i, carry):
            sa, sb, sc = carry
            rws = pl.ds(pl.multiple_of(i * TILE, TILE), TILE)
            v = res[j, rws, :] + sx[j, rws, :].astype(F32) + rx[0, j, rws, :].astype(F32) + bias
            cen = v - jnp.mean(v, axis=1, keepdims=True)
            r = lax.rsqrt(jnp.mean(cen * cen, axis=1, keepdims=True) + EPS)
            n = cen * r
            xt[rws, :] = (n * gain + shift).astype(BF)
            dz = ct[j, rws, :].astype(F32)
            dt = back_tile(dz, n, r, gain)
            res[j, rws, :] = dt
            ct[j, rws, :] = dt.astype(BF)
            return sa + fold(dz * n), sb + fold(dz), sc + fold(dt)

        zero = jnp.zeros((8, 1024), F32)
        sa, sb, sc = lax.fori_loop(0, rows // TILE, body, (zero, zero, zero))
        add_small(2, sa)
        add_small(11, sb)
        add_small(8, sc)

        @pl.when(x == j)
        def _():
            local(xt, block_out).wait()

    def units_back(j):
        def body(step, carry):
            q, i = step // 4, step % 4
            lanes = pl.ds(pl.multiple_of(i * 256, 256), 256)
            g = dot(ct[j], ws[q, :, :, :, lanes].reshape(1024, 256), 1, 0)
            g = (g * gp[q, j, :, lanes].astype(F32)).astype(BF)
            gp[q, j, :, lanes] = g
            sm[pl.ds(13 + 2 * x + q, 1), lanes] += jnp.sum(g.astype(F32), axis=0, keepdims=True)
            return carry

        lax.fori_loop(0, 8, body, 0)
        units_out(j, gp, we)
        exchange(3, j)

    last_norm(0)
    units_back(0)
    last_norm(1)
    units_back(1)

    def grad_into(dst, pieces, first=0):
        def body(i, carry):
            lanes = pl.ds(pl.multiple_of(i * 256, 256), 256)
            lo = first
            for left, right in pieces:
                g = dot(left[:, :, lanes].reshape(512, 256), right, 0, 0)
                w = g.shape[1]
                dst[pl.ds(i * nq, nq), :, :, lo : lo + w] = g.astype(BF).reshape(nq, 2, sh, w)
                lo += w
            return carry

        lax.fori_loop(0, 4, body, 0)

    own_of = {0: own.at[0], 1: own.at[1], 2: we.at[0], 3: we.at[1]}
    send_of = {0: ws.at[0], 1: ws.at[1], 2: ws.at[0], 3: ws.at[1]}
    units = [(0, 0, 1024), (1, 0, 1024), (2, 0, 256), (2, 256, 1024)] + [(3, 256 * p, 256 * p + 256) for p in range(4)]
    z_to = {k: lax.rem(z + k, nz) for k in peers_z}
    gsend, gy, gz_ = [], [], []
    for g, lo, hi in units:
        gsend.append(plan(send_of[g].at[:, :, :, lo:hi], cland.at[g, :, :, :, lo:hi], c_dev))
        gy.append(plan(own_of[g].at[:, ny, :, lo:hi], yland.at[g, :, :, lo:hi], y_dev))
        gz_.append([plan(own_of[g].at[z_to[k], y, :, lo:hi], zland.at[g, k, :, lo:hi], z_dev(k)) for k in peers_z])

    def unit_pair(ref, q):
        return ref[q].reshape(512, 1024)

    for g in ("e", "s"):
        for kind in (zc, yc, cz, cy):
            for cp in kind[g].values():
                sent(cp)
    grad_into(send_of[0], [(x2r, unit_pair(gp, nc))])
    launch(gsend[0])
    grad_into(own_of[0], [(x2r, unit_pair(gp, c))])
    grad_into(send_of[1], [(ct, unit_pair(gg, nc))])
    launch(gsend[1])
    grad_into(own_of[1], [(ct, unit_pair(gg, c))])
    l_en2a = local(enc, x2r.at[x])
    l_en2b = local(eland.at[nx], x2r.at[nx])


    def grad_core(u):
        g, lo, hi = units[u]
        gsend[u].wait_recv()
        local(cland.at[g, :, :, :, lo:hi], tmp.at[:, :, :, lo:hi]).wait()
        o = own_of[g]

        def body(i, carry):
            blk = pl.ds(i * nq, nq)
            o[blk, :, :, lo:hi] = (o[blk, :, :, lo:hi].astype(F32) + tmp[blk, :, :, lo:hi].astype(F32)).astype(BF)
            return carry

        lax.fori_loop(0, 4, body, 0)
        launch(gy[u])

    def grad_y(u):
        g, lo, hi = units[u]
        gy[u].wait_recv()
        local(yland.at[g, :, :, lo:hi], tmp.at[:, 0, :, lo:hi]).wait()
        o = own_of[g]

        def body(i, carry):
            blk = pl.ds(i * nq, nq)
            o[blk, y, :, lo:hi] = (o[blk, y, :, lo:hi].astype(F32) + tmp[blk, 0, :, lo:hi].astype(F32)).astype(BF)
            return carry

        lax.fori_loop(0, 4, body, 0)
        for cp in gz_[u]:
            launch(cp)

    out_copies = {}

    def grad_z(u, out):
        g, lo, hi = units[u]
        cps = []
        for k in peers_z:
            gz_[u][k - 1].wait_recv()
            cps.append(local(zland.at[g, k, :, lo:hi], tmp.at[k, 0, :, lo:hi]))
        for cp in cps:
            cp.wait()
        acc = own_of[g][z, y, :, lo:hi].astype(F32)
        for k in peers_z:
            acc = acc + tmp[k, 0, :, lo:hi].astype(F32)
        spot = outf.at[g % 2, :, lo:hi]
        for key in [key for key in out_copies if key[0] == g - 2]:
            out_copies.pop(key).wait()
        spot[...] = acc
        if g == 0:
            local(spot, out.at[:, lo:hi]).wait()
        else:
            out_copies[g, lo] = local(spot, out.at[:, lo:hi])

    def sum_rows(row, src, col):
        sm[row : row + 1, pl.ds(pl.multiple_of(col, 256), 256)] += jnp.sum(src.astype(F32), axis=0, keepdims=True)

    def heads_back(j, buf, lo, q_ref, k_ref, v_ref, o_ref, l_ref, causal, hooks):
        def body(q, carry):
            do[:, pl.ds(pl.multiple_of(q * 256, 256), 256)] = dot(ct[j], w_all(buf, q, lo, lo + 256), 1, 0).astype(BF)
            return carry

        lax.fori_loop(0, 2, body, 0)
        attend_back(j, q_ref, k_ref, v_ref, o_ref, l_ref, causal, hooks)

    def swap_kv(slot):
        for j in range(2):
            ksend[0, j] = dk[2 * j + nc].astype(BF)
            ksend[1, j] = dv[2 * j + nc].astype(BF)
        return send(ksend, krecv.at[slot], c_dev)

    def join_kv(slot):
        for j in range(2):
            krecv[slot, 0, j] = (dk[2 * j + c] + krecv[slot, 0, j].astype(F32)).astype(BF)
            krecv[slot, 1, j] = (dv[2 * j + c] + krecv[slot, 1, j].astype(F32)).astype(BF)

    def head_cols(ref, q):
        return ref[:, :, pl.ds(pl.multiple_of(q * 256, 256), 256)].reshape(512, 256)

    def cross_back(j, hooks):
        arrived(3, j)
        norm_back(j, 3, gains[1], n2, r2, 1, 10, 7)
        if j == 1:
            sent(gsend[0])
            grad_into(send_of[2], [(ct, head_cols(a2, nc))])
            launch(gsend[2])
            grad_into(own_of[2], [(ct, head_cols(a2, c))])
        heads_back(j, wc, 256, q2, k2, v2, a2, lse2, False, hooks)
        project_out(j, dq, wc, 0)
        exchange(4, j)

    part = functools.partial
    grad_core(0)
    cross_back(0, ({}, {2: part(grad_core, 1)}))
    cross_back(1, ({6: part(grad_y, 0)}, {4: part(grad_core, 2)}))
    swap2 = swap_kv(0)
    for j in range(2):
        for q in range(2):
            sum_rows(5, dq[j, :, q * 256 : q * 256 + 256], x * 512 + q * 256)
    swap2.wait_recv()
    join_kv(0)
    for j in range(2):
        for q in range(2):
            sum_rows(6, krecv[0, 1, j, :, q * 256 : q * 256 + 256], x * 512 + q * 256)
    l_en2a.wait()
    l_en2b.wait()

    def cross_pieces(q):
        return [
            (x1r, head_cols(dq, q)),
            (x2r, head_cols(krecv.at[0, 0], q)),
            (x2r, head_cols(krecv.at[0, 1], q)),
        ]

    grad_into(send_of[2], cross_pieces(nc), 256)
    launch(gsend[3])
    grad_into(own_of[2], cross_pieces(c), 256)
    l_x2a = local(hid, x1r.at[x])
    l_x2b = local(xland.at[nx], x1r.at[nx])

    def input_part(j, terms, dn):
        acc = None
        for ref, buf, lo in terms:
            for q in range(2):
                part = dot(ref[j, :, q * 256 : q * 256 + 256], rows_at(buf, q, dn, lo, lo + 256), 1, 1)
                acc = part if acc is None else acc + part
        return acc

    enc_terms = [(krecv.at[0, 0], wb, 256), (krecv.at[0, 1], wb, 512)]
    def part_of_enc_terms_xt(dn, cols):
        xt[:, cols] = input_part(nx, enc_terms, dn).astype(BF)

    over_columns(part_of_enc_terms_xt)
    def part_of_enc_terms_den(dn, cols):
        den[:, cols] = input_part(x, enc_terms, dn)

    over_columns(part_of_enc_terms_den)
    enc_x = send(xt, rxd.at[0], x_dev)

    def self_back(j, hooks):
        arrived(4, j)
        norm_back(j, 4, gains[0], n1, r1, 0, 9, 12)
        if j == 1:
            sent(gsend[1])
            grad_into(send_of[3], [(ct, head_cols(ao, nc))])
            launch(gsend[4])
            grad_into(own_of[3], [(ct, head_cols(ao, c))])
        heads_back(j, wb, 0, qs, ks, vs, ao, lse1, True, hooks)

    self_back(0, ({1: part(grad_core, 3), 6: part(grad_y, 1)}, {6: part(grad_y, 2)}))
    sent(enc_x)
    self_back(1, ({5: part(grad_core, 4)}, {2: part(grad_z, 0, ge_out)}))
    sent(swap2)
    swap1 = swap_kv(1)
    l_x2a.wait()
    l_x2b.wait()
    grad_into(send_of[3], [(x1r, head_cols(dq, nc))], 256)
    launch(gsend[5])
    grad_into(own_of[3], [(x1r, head_cols(dq, c))], 256)
    for j in range(2):
        for q in range(2):
            sum_rows(3, dq[j, :, q * 256 : q * 256 + 256], x * 512 + q * 256)
    swap1.wait_recv()
    join_kv(1)
    grad_into(send_of[3], [(x1r, head_cols(krecv.at[1, i], nc)) for i in range(2)], 512)
    launch(gsend[6])
    launch(gsend[7])
    grad_core(5)
    grad_y(3)
    in_terms = [(dq, wa, 0), (krecv.at[1, 0], wa, 256), (krecv.at[1, 1], wa, 512)]
    def part_of_in_terms_xt(dn, cols):
        xt[:, cols] = input_part(nx, in_terms, dn).astype(BF)

    over_columns(part_of_in_terms_xt)
    hid_x = send(xt, rxd.at[1], x_dev)
    grad_into(own_of[3], [(x1r, head_cols(krecv.at[1, i], c)) for i in range(2)], 512)
    grad_core(6)
    grad_core(7)
    for j in range(2):
        for q in range(2):
            sum_rows(4, krecv[1, 1, j, :, q * 256 : q * 256 + 256], x * 512 + q * 256)
    s1 = send(sm, smr.at[0], c_dev)
    grad_y(4)
    def part_of_in_terms_res(dn, cols):
        res[x, :, cols] += input_part(x, in_terms, dn)

    over_columns(part_of_in_terms_res)
    s1.wait_recv()
    sent(s1)
    sm[...] += smr[0]
    s2 = send(sm, smr.at[1], x_dev)
    sent(hid_x)
    enc_x.wait_recv()
    den[...] += rxd[0].astype(F32)
    o1 = local(den, enc_out)
    grad_y(5)
    s2.wait_recv()
    sent(s2)
    sm[...] += smr[1]
    s3 = send(sm, smr.at[2], y_dev)
    grad_z(1, gs_out)
    hid_x.wait_recv()
    res[x] += rxd[1].astype(F32)
    o2 = local(res.at[x], hid_out)
    grad_y(6)
    s3.wait_recv()
    sent(s3)
    sm[...] += smr[2]
    smz[z] = sm[...]
    s4 = [send(sm, smz.at[z], z_dev(k)) for k in range(1, nz)]
    grad_y(7)
    grad_z(2, gc_out)
    grad_z(3, gc_out)
    grad_z(4, ga_out)
    grad_z(5, ga_out)
    for cp in s4:
        cp.wait_recv()
        sent(cp)
    acc = smz[0]
    for k in range(1, nz):
        acc = acc + smz[k]
    for row in range(3):
        gain_out[row] = acc[row : row + 1, :]
    for row in range(9):
        bias_out[row] = acc[row + 3 : row + 4, :]
    selfb_out[...] = acc[12:13, :]
    for row in range(4):
        expb_out[:, row * 1024 : row * 1024 + 1024] = acc[row + 13 : row + 14, :]
    grad_z(6, ga_out)
    grad_z(7, ga_out)
    for cp in [o1, o2] + list(out_copies.values()):
        cp.wait()
    for cp in list(pending):
        sent(cp)


def run_layer(nz, sh, prefix, hid, enc, cot, shards, gains, biases, selfb, expb):
    any_spec = pl.BlockSpec(memory_space=pl.ANY)
    vmem = pl.BlockSpec(memory_space=pltpu.VMEM)
    rows = hid.shape[0]
    shape = jax.ShapeDtypeStruct
    outs = [
        shape((rows, 1024), BF),
        shape((rows, 1024), F32),
        shape((rows, 1024), F32),
        shape((sh, 1024), F32),
        shape((sh, 1024), F32),
        shape((sh, 1024), F32),
        shape((sh, 1024), F32),
        shape((3, 1, 1024), F32),
        shape((9, 1, 1024), F32),
        shape((1, 1024), F32),
        shape((1, 4096), F32),
        shape((2, rows, 1024), BF),
        shape((2, rows, 1024), BF),
        shape((4, nz, 2, sh, 1024), BF),
        shape((4, nz, sh, 1024), BF),
        shape((4, nz, sh, 1024), BF),
    ]

    def weight(n):
        return pltpu.VMEM((2, nz, 2, sh, n), BF)

    def acts(n, kind=BF):
        return pltpu.VMEM((2, rows, n), kind)

    def keys(kind=BF):
        return pltpu.VMEM((4, rows, 512), kind)

    scratch = [
        weight(768),
        weight(768),
        weight(512),
        weight(1024),
        weight(1024),
        acts(1024),
        acts(1024),
        acts(1024),
        acts(512),
        keys(),
        keys(),
        acts(512),
        acts(512),
        keys(),
        keys(),
        acts(512),
        pltpu.VMEM((2, 2, rows, 1024), BF),
        pltpu.VMEM((2, 2, rows, 1024), BF),
        acts(1024),
        acts(1024),
        acts(128, F32),
        acts(128, F32),
        acts(128, F32),
        acts(128, F32),
        acts(1024, F32),
        acts(1024),
        pltpu.VMEM((2, 2, rows, 1024), BF),
        acts(1024),
        acts(512),
        pltpu.VMEM((rows, 512), BF),
        keys(F32),
        keys(F32),
        pltpu.VMEM((2, 2, rows, 512), BF),
        pltpu.VMEM((2, 2, 2, rows, 512), BF),
        pltpu.VMEM((2, 1024, 1024), BF),
        pltpu.VMEM((2, nz, 2, sh, 1024), BF),
        pltpu.VMEM((nz, 2, sh, 1024), BF),
        pltpu.VMEM((rows, 1024), BF),
        pltpu.VMEM((1024, 256), BF),
        pltpu.VMEM((1024, 256), BF),
        pltpu.VMEM((rows, 1024), F32),
        pltpu.VMEM((2, sh, 1024), F32),
        pltpu.VMEM((SMALL_ROWS, 1024), F32),
        pltpu.VMEM((3, SMALL_ROWS, 1024), F32),
        pltpu.VMEM((nz, SMALL_ROWS, 1024), F32),
        pltpu.SemaphoreType.DMA((280 + 64 * nz,)),
    ]
    return pl.pallas_call(
        functools.partial(layer_kernel, nz, sh),
        out_shape=outs,
        in_specs=[pl.BlockSpec(memory_space=pltpu.SMEM)] + [any_spec] * 13 + [vmem] * 4,
        out_specs=[any_spec] * 7 + [vmem] * 4 + [any_spec] * (len(outs) - 11),
        scratch_shapes=scratch,
        compiler_params=pltpu.CompilerParams(
            collective_id=0, has_side_effects=True, vmem_limit_bytes=67043328
        ),
    )(prefix, hid, enc, cot, *shards, gains, biases, selfb, expb)


def per_device(
    hidden,
    encoder,
    prefix,
    query_self,
    key_self,
    value_self,
    output_self,
    cross_query_matrix,
    key_cross,
    value_cross,
    output_cross,
    expand,
    shrink,
    norm_gains,
    biases,
    self_out_bias,
    expand_bias,
    cotangent,
):
    sh = query_self.shape[1]
    nz = 1024 // sh // 2
    shards = (
        query_self[0],
        key_self[0],
        value_self[0],
        output_self[0].T,
        key_cross[0],
        value_cross[0],
        cross_query_matrix[0],
        output_cross[0].T,
        expand[0],
        shrink[0].T,
    )
    outs = run_layer(
        nz,
        sh,
        prefix,
        hidden[0],
        encoder[0],
        cotangent[0],
        shards,
        jnp.swapaxes(norm_gains, 0, 1),
        jnp.swapaxes(biases, 0, 1),
        self_out_bias,
        expand_bias,
    )
    block, grad_hid, grad_enc, ge, gs, gc, ga, gain, bias, selfb, expb = outs[:11]

    def part(g, i):
        return g[:, i * 256 : i * 256 + 256]

    return (
        block[None],
        grad_hid[None],
        grad_enc[None],
        part(ga, 1)[None],
        part(ga, 2)[None],
        part(ga, 3)[None],
        part(ga, 0).T[None],
        part(gc, 1)[None],
        part(gc, 2)[None],
        part(gc, 3)[None],
        part(gc, 0).T[None],
        ge[None],
        gs.T[None],
        jnp.swapaxes(gain, 0, 1),
        jnp.swapaxes(bias, 0, 1),
        selfb,
        expb,
    )


def solution(mesh):
    in_specs = (
        P("dp", "tensor", None),
        P("dp", "tensor", None),
        P("dp"),
        P(None, "dp", "tensor"),
        P(None, "dp", "tensor"),
        P(None, "dp", "tensor"),
        P(None, "tensor", "dp"),
        P(None, "dp", "tensor"),
        P(None, "dp", "tensor"),
        P(None, "dp", "tensor"),
        P(None, "tensor", "dp"),
        P(None, "dp", "tensor"),
        P(None, "tensor", "dp"),
        P(),
        P(),
        P(),
        P(),
        P("dp", "tensor", None),
    )
    out_specs = (
        P("dp", "tensor", None),
        P("dp", "tensor", None),
        P("dp", "tensor", None),
        P(None, "dp", "tensor"),
        P(None, "dp", "tensor"),
        P(None, "dp", "tensor"),
        P(None, "tensor", "dp"),
        P(None, "dp", "tensor"),
        P(None, "dp", "tensor"),
        P(None, "dp", "tensor"),
        P(None, "tensor", "dp"),
        P(None, "dp", "tensor"),
        P(None, "tensor", "dp"),
        P(),
        P(),
        P(),
        P(),
    )
    return jax.shard_map(
        per_device, mesh=mesh, in_specs=in_specs, out_specs=out_specs, check_vma=False
    )
```

```python
import functools

import jax
import jax.numpy as jnp
from jax import lax
from jax.experimental import pallas as pl
from jax.experimental.pallas import tpu as pltpu
from jax.sharding import PartitionSpec as P

MESH = pl.DeviceIdType.MESH
BF = jnp.bfloat16
F32 = jnp.float32
EPS = 1e-05
HEAD = 64
LOG2E = 1.4426950408889634
LN2 = 0.6931471805599453
NEG = -1e30
SMALL_ROWS = 24


def dot(a, b, ca, cb):
    return lax.dot_general(a, b, (((ca,), (cb,)), ((), ())), preferred_element_type=F32)


def layer_kernel(nz, sh, *refs):
    (
        prefix,
        hid,
        enc,
        cot,
        q_in,
        k_in,
        v_in,
        o_in,
        k2_in,
        v2_in,
        q2_in,
        o2_in,
        we_in,
        ws_in,
        gains,
        biases,
        selfb,
        expb,
        block_out,
        hid_out,
        enc_out,
        ge_out,
        gs_out,
        gc_out,
        ga_out,
        gain_out,
        bias_out,
        selfb_out,
        expb_out,
        xland,
        eland,
        cland,
        yland,
        zland,
        wa,
        wb,
        wc,
        we,
        ws,
        x1r,
        x2r,
        ct,
        qs,
        ks,
        vs,
        ao,
        q2,
        k2,
        v2,
        a2,
        gg,
        gp,
        n1,
        n2,
        r1,
        r2,
        lse1,
        lse2,
        res,
        sx,
        rx,
        rxd,
        dq,
        do,
        dk,
        dv,
        ksend,
        krecv,
        cs,
        own,
        tmp,
        xt,
        dom,
        qm,
        den,
        outf,
        sm,
        smr,
        smz,
        sems,
    ) = refs
    d = lax.axis_index("dp")
    t = lax.axis_index("tensor")
    x, c = t // 2, t % 2
    z, y = d // 2, d % 2
    nx, nc, ny = 1 - x, 1 - c, 1 - y
    x_dev = (d, nx * 2 + c)
    c_dev = (d, x * 2 + nc)
    y_dev = (z * 2 + ny, t)

    def z_dev(k):
        return (lax.rem(z + k, nz) * 2 + y, t)

    def z_from(k):
        return lax.rem(z + nz - k, nz)

    nq = nz // 4
    rows = hid.shape[0]
    count = [0]

    def new_sem():
        count[0] += 1
        return sems.at[count[0] - 1]

    pending = []

    def plan(src, dst, dev):
        return pltpu.make_async_remote_copy(
            src_ref=src, dst_ref=dst, send_sem=new_sem(), recv_sem=new_sem(), device_id=dev, device_id_type=MESH
        )

    def launch(cp):
        cp.start()
        pending.append(cp)
        return cp

    def send(src, dst, dev):
        return launch(plan(src, dst, dev))

    def sent(cp):
        cp.wait_send()
        pending[:] = [other for other in pending if other is not cp]

    def local(src, dst):
        cp = pltpu.make_async_copy(src, dst, new_sem())
        cp.start()
        return cp

    barrier = pltpu.get_barrier_semaphore()
    peers = [x_dev, c_dev, y_dev] + [z_dev(k) for k in range(1, nz)]
    for dev in peers:
        pl.semaphore_signal(barrier, inc=1, device_id=dev, device_id_type=MESH)
    pl.semaphore_wait(barrier, len(peers))

    xs = [send(hid, xland.at[x], x_dev)]
    groups = {
        "a": ([q_in, k_in, v_in], wa),
        "b": ([o_in, k2_in, v2_in], wb),
        "c": ([q2_in, o2_in], wc),
        "e": ([we_in], we),
        "s": ([ws_in], ws),
    }

    class Bundle:
        def __init__(self, copies):
            self.copies = copies

        def start(self):
            for cp in self.copies:
                cp.start()

        def wait_recv(self):
            for cp in self.copies:
                cp.wait_recv()

        def wait_send(self):
            for cp in self.copies:
                cp.wait_send()

        def wait(self):
            for cp in self.copies:
                cp.wait()

    def columns_of(srcs, g, spot):
        width = srcs[0].shape[1]
        buf = groups[g][1]
        for i, src in enumerate(srcs):
            yield src, buf.at[(*spot, slice(None), slice(i * width, i * width + width))]

    def plan_own(g, dev):
        return Bundle([plan(src, dst, dev) for src, dst in columns_of(groups[g][0], g, (c, z, y))])

    zc, yc, cz, cy, lc = {}, {}, {}, {}, {}
    peers_z = range(1, nz)

    for g in groups:
        buf = groups[g][1]
        zc[g] = {k: plan_own(g, z_dev(k)) for k in peers_z}
        yc[g] = {0: plan_own(g, y_dev)}
        cz[g] = {0: plan_own(g, c_dev)}
        cy[g] = {}
        for k in range(nz):
            zk = z_from(k)
            if k:
                spot = buf.at[c, zk, y]
                yc[g][k] = plan(spot, spot, y_dev)
                cz[g][k] = plan(spot, spot, c_dev)
            spot = buf.at[c, zk, ny]
            cy[g][k] = plan(spot, spot, c_dev)

    def start_z(g):
        for k in peers_z:
            launch(zc[g][k])

    def start_y(g):
        launch(yc[g][0])

    def start_c(g):
        launch(cz[g][0])
        lc[g] = Bundle([local(src, dst) for src, dst in columns_of(groups[g][0], g, (c, z, y))])

    def thirds(part):
        return range(1 + (nz - 1) * part // 3, 1 + (nz - 1) * (part + 1) // 3)

    def z_event(g, part):
        for k in thirds(part):
            zc[g][k].wait_recv()
            launch(yc[g][k])
            launch(cz[g][k])

    def y_event(g, part):
        for k in [0] if part < 0 else thirds(part):
            yc[g][k].wait_recv()
            launch(cy[g][k])

    def c_event(g):
        lc[g].wait()
        for cp in list(cz[g].values()) + list(cy[g].values()):
            cp.wait_recv()

    def run(*words):
        for word in words:
            kind, g, part = word[0], word[1], int(word[2:] or 0)
            if kind == "o":
                start_y(g)
            else:
                (z_event if kind == "z" else y_event)(g, part)

    start_z("a")
    start_y("a")
    start_c("a")
    l_x = local(hid, x1r.at[x])
    l_e = local(enc, x2r.at[x])
    l_c = local(cot, ct.at[x])
    start_z("b")
    start_y("b")
    start_c("b")
    xs.append(send(enc, eland.at[x], x_dev))
    xs.append(send(cot, ct.at[x], x_dev))
    for g in ("c", "e", "s"):
        start_z(g)
        start_c(g)

    def hooked(hooks, i):
        for at, text in hooks.items():
            if isinstance(text, tuple):
                pl.when(i == at // 2 * 2)(functools.partial(run, *text))
            else:
                pl.when(i == at // 2 * 2)(text)

    def w_all(buf, q, lo, hi):
        return buf[q, :, :, :, lo:hi].reshape(1024, hi - lo)

    def bias_at(ref, row, lo, width):
        return ref[row, :, pl.ds(pl.multiple_of(lo, 256), width)]

    sm[...] = jnp.zeros_like(sm)

    def fold(v):
        return jnp.sum(v.reshape(v.shape[0] // 8, 8, v.shape[1]), axis=0)

    scale = HEAD**-0.5

    l_x.wait()
    xs[0].wait_recv()
    l_xn = local(xland.at[nx], x1r.at[nx])
    run("za0", "ya-1", "za1", "ya0", "za2", "oc", "ya1", "ya2")
    l_xn.wait()
    c_event("a")
    kv1 = []
    for j in range(2):
        xj = x1r[j]
        for q in range(2):
            r = dot(xj, w_all(wa, q, 0, 768), 1, 0)
            lanes = slice(q * 256, q * 256 + 256)
            col = x * 512 + q * 256
            qs[j, :, lanes] = ((r[:, :256] + bias_at(biases, 0, col, 256)) * (scale * LOG2E)).astype(BF)
            ks[2 * j + c, :, lanes] = r[:, 256:512].astype(BF)
            vs[2 * j + c, :, lanes] = (r[:, 512:] + bias_at(biases, 1, col, 256)).astype(BF)
        kv1 += [send(b.at[2 * j + c], b.at[2 * j + c], c_dev) for b in (ks, vs)]
        run(*(("zb0", "oe") if j == 0 else ("zb1",)))
    xs[1].wait_recv()
    l_en = local(eland.at[nx], x2r.at[nx])

    lane256 = lax.broadcasted_iota(jnp.int32, (128, 256), 1)
    lane128 = lax.broadcasted_iota(jnp.int32, (128, 128), 1)
    zero_bf = jnp.zeros((128, 256), BF)
    lane256w = lax.broadcasted_iota(jnp.int32, (256, 256), 1)
    lane128w = lax.broadcasted_iota(jnp.int32, (256, 128), 1)
    zero_bfw = jnp.zeros((256, 256), BF)
    limit = prefix[0]

    def parts_of(keys, causal, j):
        if not causal:
            return [(0, 4, False)]
        return [(0, 2, True)] if j == 0 else [(0, 2, False), (2, 4, True)]

    def scores(qh, k_ref, part, lanes, j, row0):
        b0, b1, masked = part
        k = k_ref[b0:b1, :, lanes].reshape((b1 - b0) * 256, 256)
        s = dot(qh, k, 1, 1)
        if masked:
            cols = b0 * 256 + lax.broadcasted_iota(jnp.int32, s.shape, 1)
            rws = (2 * j + c) * 256 + row0 + lax.broadcasted_iota(jnp.int32, s.shape, 0)
            s = jnp.where((cols <= rws) | (cols < limit), s, NEG)
        return s

    def attend(j, q_ref, k_ref, v_ref, o_ref, l_ref, causal, hooks):
        parts = parts_of(k_ref, causal, j)

        def body(i, carry):
            hooked(hooks, 2 * i)
            h = i
            row0 = 0
            rws = slice(0, 256)
            lanes = pl.ds(pl.multiple_of((h // 4) * 256, 256), 256)
            head = (lane256w // HEAD) == (h % 4)
            qh = jnp.where(head, q_ref[j, rws, lanes], zero_bfw)
            ss = [scores(qh, k_ref, p, lanes, j, row0) for p in parts]
            m = functools.reduce(jnp.maximum, [jnp.max(s, axis=1, keepdims=True) for s in ss])
            total = jnp.zeros((256, 1), F32)
            o = jnp.zeros((256, 256), F32)
            for s, (b0, b1, _) in zip(ss, parts):
                p = jnp.exp2(s - m)
                total = total + jnp.sum(p, axis=1, keepdims=True)
                o = o + dot(p.astype(BF), v_ref[b0:b1, :, lanes].reshape((b1 - b0) * 256, 256), 1, 0)
            o = o / total
            o_ref[j, rws, lanes] = jnp.where(head, o.astype(BF), o_ref[j, rws, lanes])
            l_ref[j, rws, :] = jnp.where(lane128w == h, m + jnp.log2(total), l_ref[j, rws, :])
            return carry

        lax.fori_loop(0, 8, body, 0)

    def attend_back(j, q_ref, k_ref, v_ref, o_ref, l_ref, causal, hooks):
        parts = parts_of(k_ref, causal, j)
        nk = 256 * parts[-1][1]
        for qt in range(2):
            lanes = slice(qt * 256, qt * 256 + 256)

            def body(i, carry):
                hooked(hooks[qt], 2 * i)
                h = i
                row0 = 0
                rws = slice(0, 256)
                spot = pl.ds(pl.multiple_of(i * 256, 256), 256)
                head = (lane256w // HEAD) == h
                qh = jnp.where(head, q_ref[j, rws, lanes], zero_bfw)
                dh = jnp.where(head, do[rws, lanes], zero_bfw)
                delta = jnp.sum(dh.astype(F32) * o_ref[j, rws, lanes].astype(F32), axis=1, keepdims=True)
                lse = jnp.sum(jnp.where(lane128w == h + 4 * qt, l_ref[j, rws, :], 0.0), axis=1, keepdims=True)
                g = jnp.zeros((256, 256), F32)
                for part in parts:
                    b0, b1, _ = part
                    s = scores(qh, k_ref, part, lanes, j, row0)
                    p = jnp.exp2(s - lse)
                    dp = dot(dh, v_ref[b0:b1, :, lanes].reshape((b1 - b0) * 256, 256), 1, 1)
                    ds = (p * (dp - delta)).astype(BF)
                    cs[0, spot, b0 * 256 : b1 * 256] = p.astype(BF)
                    cs[1, spot, b0 * 256 : b1 * 256] = ds
                    g = g + dot(ds, k_ref[b0:b1, :, lanes].reshape((b1 - b0) * 256, 256), 1, 0)
                dq[j, rws, lanes] = jnp.where(head, (g.astype(BF) * scale).astype(BF), dq[j, rws, lanes])
                dom[spot, :] = dh
                qm[spot, :] = qh
                return carry

            lax.fori_loop(0, 4, body, 0)
            for b in range(nk // 256):
                keys = slice(b * 256, b * 256 + 256)
                gv = dot(cs[0, :, keys], dom[...], 0, 0)
                gk = dot(cs[1, :, keys], qm[...], 0, 0) * LN2
                if j == 0:
                    dv[b, :, lanes] = gv
                    dk[b, :, lanes] = gk
                else:
                    dv[b, :, lanes] += gv
                    dk[b, :, lanes] += gk
        if j == 0 and nk < 1024:
            dv[2:4] = jnp.zeros((2, 256, 512), F32)
            dk[2:4] = jnp.zeros((2, 256, 512), F32)

    def over_columns(body):
        def step(dn, carry):
            body(dn, pl.ds(pl.multiple_of(dn * 256, 256), 256))
            return carry

        lax.fori_loop(0, 4, step, 0)

    def rows_at(buf, q, dn, lo, hi):
        return buf[q, pl.ds(dn * nq, nq), :, :, lo:hi].reshape(256, hi - lo)

    def project_out(j, src, buf, lo):
        def body(dn, cols):
            acc = dot(src[j, :, 0:256], rows_at(buf, 0, dn, lo, lo + 256), 1, 1)
            acc = acc + dot(src[j, :, 256:512], rows_at(buf, 1, dn, lo, lo + 256), 1, 1)
            sx[j, :, cols] = acc.astype(BF)

        over_columns(body)

    ex = {}

    def exchange(stage, j):
        ex[stage, j] = send(sx.at[j], rx.at[stage % 2, j], x_dev)

    def arrived(stage, j):
        ex[stage, j].wait_recv()
        sent(ex[stage, j])

    TILE = 32

    def norm_forward(j, stage, base, bias, gain, shift, n_ref, r_ref, low_ref):
        def body(i, carry):
            rws = pl.ds(pl.multiple_of(i * TILE, TILE), TILE)
            v = base[j, rws, :].astype(F32) + sx[j, rws, :].astype(F32) + rx[stage % 2, j, rws, :].astype(F32) + bias
            cen = v - jnp.mean(v, axis=1, keepdims=True)
            r = lax.rsqrt(jnp.mean(cen * cen, axis=1, keepdims=True) + EPS)
            n = cen * r
            o = n * gain + shift
            n_ref[j, rws, :] = n.astype(BF)
            r_ref[j, rws, :] = jnp.broadcast_to(r, (TILE, 128))
            res[j, rws, :] = o
            low_ref[j, rws, :] = o.astype(BF)
            return carry

        lax.fori_loop(0, rows // TILE, body, 0)

    def add_small(row, v):
        sm[row : row + 1, :] += jnp.sum(v, axis=0, keepdims=True) * 0.5

    def back_tile(dz, n, r, gain):
        gz = gain * dz
        ma = jnp.mean(gz, axis=1, keepdims=True)
        mb = jnp.mean(gz * n, axis=1, keepdims=True)
        return (gz - ma - n * mb) * r

    def norm_back(j, stage, gain, n_ref, r_ref, gain_row, shift_row, bias_row):
        def body(i, carry):
            sa, sb, sc = carry
            rws = pl.ds(pl.multiple_of(i * TILE, TILE), TILE)
            dz = res[j, rws, :] + sx[j, rws, :].astype(F32) + rx[stage % 2, j, rws, :].astype(F32)
            n = n_ref[j, rws, :].astype(F32)
            dt = back_tile(dz, n, r_ref[j, rws, 0:1], gain)
            res[j, rws, :] = dt
            ct[j, rws, :] = dt.astype(BF)
            return sa + fold(dz * n), sb + fold(dz), sc + fold(dt)

        zero = jnp.zeros((8, 1024), F32)
        sa, sb, sc = lax.fori_loop(0, rows // TILE, body, (zero, zero, zero))
        add_small(gain_row, sa)
        add_small(shift_row, sb)
        add_small(bias_row, sc)

    for cp in kv1:
        cp.wait_recv()
    attend(0, qs, ks, vs, ao, lse1, True, {8: ("zb2",)})
    run("yb-1", "yb0", "zc0", "os", "yb1", "yb2")
    c_event("b")
    project_out(0, ao, wb, 0)
    exchange(0, 0)
    attend(1, qs, ks, vs, ao, lse1, True, {2: ("zc1",), 12: ("zc2",)})
    project_out(1, ao, wb, 0)
    exchange(0, 1)
    run("yc-1", "yc0")
    l_e.wait()
    l_en.wait()
    def encoder_part(i, carry):
        j, q = i // 2, i % 2
        r = dot(x2r[j], w_all(wb, q, 256, 768), 1, 0)
        lanes = pl.ds(pl.multiple_of(q * 256, 256), 256)
        k2[2 * j + c, :, lanes] = r[:, :256].astype(BF)
        v2[2 * j + c, :, lanes] = (r[:, 256:] + bias_at(biases, 3, x * 512 + q * 256, 256)).astype(BF)
        return carry

    lax.fori_loop(0, 4, encoder_part, 0)
    run("ze0", "yc1", "yc2")
    kv2 = [send(b.at[2 * j + c], b.at[2 * j + c], c_dev) for j in range(2) for b in (k2, v2)]
    c_event("c")
    for cp in kv2:
        cp.wait_recv()

    def cross(j, hooks):
        arrived(0, j)
        norm_forward(j, 0, x1r, selfb[0:1, :], gains[0], biases[6], n1, r1, x1r)

        def body(q, carry):
            r = dot(x1r[j], w_all(wc, q, 0, 256), 1, 0) + bias_at(biases, 2, x * 512 + q * 256, 256)
            q2[j, :, pl.ds(pl.multiple_of(q * 256, 256), 256)] = (r * (scale * LOG2E)).astype(BF)
            return carry

        lax.fori_loop(0, 2, body, 0)
        attend(j, q2, k2, v2, a2, lse2, False, hooks)
        project_out(j, a2, wc, 256)
        exchange(1, j)

    cross(0, {4: ("ze1",), 14: ("ze2",)})
    cross(1, {4: ("ye-1", "ye0", "zs0",), 14: ("zs1", "ye1")})

    root_half = 0.7071067811865476
    norm_pdf = 0.3989422804014327

    def hidden_units(j):
        arrived(1, j)
        norm_forward(j, 1, res, biases[4], gains[1], biases[7], n2, r2, x2r)

        def body(step, carry):
            q, i = step // 4, step % 4
            lanes = pl.ds(pl.multiple_of(i * 256, 256), 256)
            h = dot(x2r[j], we[q, :, :, :, lanes].reshape(1024, 256), 1, 0)
            h = h + expb[0:1, pl.ds(pl.multiple_of(x * 2048 + step * 256, 256), 256)]
            cdf = 0.5 * (1.0 + lax.erf(h * root_half))
            gg[q, j, :, lanes] = (h * cdf).astype(BF)
            gp[q, j, :, lanes] = (cdf + h * (jnp.exp(-0.5 * h * h) * norm_pdf)).astype(BF)
            return carry

        lax.fori_loop(0, 8, body, 0)

    def units_out(j, src, buf):
        def body(dn, cols):
            acc = dot(src[0, j], rows_at(buf, 0, dn, 0, 1024), 1, 1)
            acc = acc + dot(src[1, j], rows_at(buf, 1, dn, 0, 1024), 1, 1)
            sx[j, :, cols] = acc.astype(BF)

        over_columns(body)

    run("ye2")
    c_event("e")
    hidden_units(0)
    run("zs2", "ys-1", "ys0")
    hidden_units(1)
    run("ys1", "ys2")
    c_event("s")
    units_out(0, gg, ws)
    exchange(2, 0)
    units_out(1, gg, ws)
    exchange(2, 1)
    l_c.wait()
    xs[2].wait_recv()

    def last_norm(j):
        arrived(2, j)
        gain, shift, bias = gains[2], biases[8], biases[5]

        def body(i, carry):
            sa, sb, sc = carry
            rws = pl.ds(pl.multiple_of(i * TILE, TILE), TILE)
            v = res[j, rws, :] + sx[j, rws, :].astype(F32) + rx[0, j, rws, :].astype(F32) + bias
            cen = v - jnp.mean(v, axis=1, keepdims=True)
            r = lax.rsqrt(jnp.mean(cen * cen, axis=1, keepdims=True) + EPS)
            n = cen * r
            xt[rws, :] = (n * gain + shift).astype(BF)
            dz = ct[j, rws, :].astype(F32)
            dt = back_tile(dz, n, r, gain)
            res[j, rws, :] = dt
            ct[j, rws, :] = dt.astype(BF)
            return sa + fold(dz * n), sb + fold(dz), sc + fold(dt)

        zero = jnp.zeros((8, 1024), F32)
        sa, sb, sc = lax.fori_loop(0, rows // TILE, body, (zero, zero, zero))
        add_small(2, sa)
        add_small(11, sb)
        add_small(8, sc)

        @pl.when(x == j)
        def _():
            local(xt, block_out).wait()

    def units_back(j):
        def body(step, carry):
            q, i = step // 4, step % 4
            lanes = pl.ds(pl.multiple_of(i * 256, 256), 256)
            g = dot(ct[j], ws[q, :, :, :, lanes].reshape(1024, 256), 1, 0)
            g = (g * gp[q, j, :, lanes].astype(F32)).astype(BF)
            gp[q, j, :, lanes] = g
            sm[pl.ds(13 + 2 * x + q, 1), lanes] += jnp.sum(g.astype(F32), axis=0, keepdims=True)
            return carry

        lax.fori_loop(0, 8, body, 0)
        units_out(j, gp, we)
        exchange(3, j)

    last_norm(0)
    units_back(0)
    last_norm(1)
    units_back(1)

    def grad_into(dst, pieces, first=0):
        def body(i, carry):
            lanes = pl.ds(pl.multiple_of(i * 256, 256), 256)
            lo = first
            for left, right in pieces:
                g = dot(left[:, :, lanes].reshape(512, 256), right, 0, 0)
                w = g.shape[1]
                dst[pl.ds(i * nq, nq), :, :, lo : lo + w] = g.astype(BF).reshape(nq, 2, sh, w)
                lo += w
            return carry

        lax.fori_loop(0, 4, body, 0)

    own_of = {0: own.at[0], 1: own.at[1], 2: we.at[0], 3: we.at[1]}
    send_of = {0: ws.at[0], 1: ws.at[1], 2: ws.at[0], 3: ws.at[1]}
    units = [(0, 0, 1024), (1, 0, 1024), (2, 0, 256), (2, 256, 1024)] + [(3, 256 * p, 256 * p + 256) for p in range(4)]
    z_to = {k: lax.rem(z + k, nz) for k in peers_z}
    gsend, gy, gz_ = [], [], []
    for g, lo, hi in units:
        gsend.append(plan(send_of[g].at[:, :, :, lo:hi], cland.at[g, :, :, :, lo:hi], c_dev))
        gy.append(plan(own_of[g].at[:, ny, :, lo:hi], yland.at[g, :, :, lo:hi], y_dev))
        gz_.append([plan(own_of[g].at[z_to[k], y, :, lo:hi], zland.at[g, k, :, lo:hi], z_dev(k)) for k in peers_z])

    def unit_pair(ref, q):
        return ref[q].reshape(512, 1024)

    for g in ("e", "s"):
        for kind in (zc, yc, cz, cy):
            for cp in kind[g].values():
                sent(cp)
    grad_into(send_of[0], [(x2r, unit_pair(gp, nc))])
    launch(gsend[0])
    grad_into(own_of[0], [(x2r, unit_pair(gp, c))])
    grad_into(send_of[1], [(ct, unit_pair(gg, nc))])
    launch(gsend[1])
    grad_into(own_of[1], [(ct, unit_pair(gg, c))])
    l_en2a = local(enc, x2r.at[x])
    l_en2b = local(eland.at[nx], x2r.at[nx])


    def grad_core(u):
        g, lo, hi = units[u]
        gsend[u].wait_recv()
        local(cland.at[g, :, :, :, lo:hi], tmp.at[:, :, :, lo:hi]).wait()
        o = own_of[g]

        def body(i, carry):
            blk = pl.ds(i * nq, nq)
            o[blk, :, :, lo:hi] = (o[blk, :, :, lo:hi].astype(F32) + tmp[blk, :, :, lo:hi].astype(F32)).astype(BF)
            return carry

        lax.fori_loop(0, 4, body, 0)
        launch(gy[u])

    def grad_y(u):
        g, lo, hi = units[u]
        gy[u].wait_recv()
        local(yland.at[g, :, :, lo:hi], tmp.at[:, 0, :, lo:hi]).wait()
        o = own_of[g]

        def body(i, carry):
            blk = pl.ds(i * nq, nq)
            o[blk, y, :, lo:hi] = (o[blk, y, :, lo:hi].astype(F32) + tmp[blk, 0, :, lo:hi].astype(F32)).astype(BF)
            return carry

        lax.fori_loop(0, 4, body, 0)
        for cp in gz_[u]:
            launch(cp)

    out_copies = {}

    def grad_z(u, out):
        g, lo, hi = units[u]
        cps = []
        for k in peers_z:
            gz_[u][k - 1].wait_recv()
            cps.append(local(zland.at[g, k, :, lo:hi], tmp.at[k, 0, :, lo:hi]))
        for cp in cps:
            cp.wait()
        acc = own_of[g][z, y, :, lo:hi].astype(F32)
        for k in peers_z:
            acc = acc + tmp[k, 0, :, lo:hi].astype(F32)
        spot = outf.at[g % 2, :, lo:hi]
        for key in [key for key in out_copies if key[0] == g - 2]:
            out_copies.pop(key).wait()
        spot[...] = acc
        if g == 0:
            local(spot, out.at[:, lo:hi]).wait()
        else:
            out_copies[g, lo] = local(spot, out.at[:, lo:hi])

    def sum_rows(row, src, col):
        sm[row : row + 1, pl.ds(pl.multiple_of(col, 256), 256)] += jnp.sum(src.astype(F32), axis=0, keepdims=True)

    def heads_back(j, buf, lo, q_ref, k_ref, v_ref, o_ref, l_ref, causal, hooks):
        def body(q, carry):
            do[:, pl.ds(pl.multiple_of(q * 256, 256), 256)] = dot(ct[j], w_all(buf, q, lo, lo + 256), 1, 0).astype(BF)
            return carry

        lax.fori_loop(0, 2, body, 0)
        attend_back(j, q_ref, k_ref, v_ref, o_ref, l_ref, causal, hooks)

    def swap_kv(slot):
        for j in range(2):
            ksend[0, j] = dk[2 * j + nc].astype(BF)
            ksend[1, j] = dv[2 * j + nc].astype(BF)
        return send(ksend, krecv.at[slot], c_dev)

    def join_kv(slot):
        for j in range(2):
            krecv[slot, 0, j] = (dk[2 * j + c] + krecv[slot, 0, j].astype(F32)).astype(BF)
            krecv[slot, 1, j] = (dv[2 * j + c] + krecv[slot, 1, j].astype(F32)).astype(BF)

    def head_cols(ref, q):
        return ref[:, :, pl.ds(pl.multiple_of(q * 256, 256), 256)].reshape(512, 256)

    def cross_back(j, hooks):
        arrived(3, j)
        norm_back(j, 3, gains[1], n2, r2, 1, 10, 7)
        if j == 1:
            sent(gsend[0])
            grad_into(send_of[2], [(ct, head_cols(a2, nc))])
            launch(gsend[2])
            grad_into(own_of[2], [(ct, head_cols(a2, c))])
        heads_back(j, wc, 256, q2, k2, v2, a2, lse2, False, hooks)
        project_out(j, dq, wc, 0)
        exchange(4, j)

    part = functools.partial
    grad_core(0)
    cross_back(0, ({}, {2: part(grad_core, 1)}))
    cross_back(1, ({}, {2: part(grad_y, 0), 6: part(grad_core, 2)}))
    swap2 = swap_kv(0)
    for j in range(2):
        for q in range(2):
            sum_rows(5, dq[j, :, q * 256 : q * 256 + 256], x * 512 + q * 256)
    swap2.wait_recv()
    join_kv(0)
    for j in range(2):
        for q in range(2):
            sum_rows(6, krecv[0, 1, j, :, q * 256 : q * 256 + 256], x * 512 + q * 256)
    l_en2a.wait()
    l_en2b.wait()

    def cross_pieces(q):
        return [
            (x1r, head_cols(dq, q)),
            (x2r, head_cols(krecv.at[0, 0], q)),
            (x2r, head_cols(krecv.at[0, 1], q)),
        ]

    grad_into(send_of[2], cross_pieces(nc), 256)
    launch(gsend[3])
    grad_into(own_of[2], cross_pieces(c), 256)
    l_x2a = local(hid, x1r.at[x])
    l_x2b = local(xland.at[nx], x1r.at[nx])

    def input_part(j, terms, dn):
        acc = None
        for ref, buf, lo in terms:
            for q in range(2):
                part = dot(ref[j, :, q * 256 : q * 256 + 256], rows_at(buf, q, dn, lo, lo + 256), 1, 1)
                acc = part if acc is None else acc + part
        return acc

    enc_terms = [(krecv.at[0, 0], wb, 256), (krecv.at[0, 1], wb, 512)]
    def part_of_enc_terms_xt(dn, cols):
        xt[:, cols] = input_part(nx, enc_terms, dn).astype(BF)

    over_columns(part_of_enc_terms_xt)
    def part_of_enc_terms_den(dn, cols):
        den[:, cols] = input_part(x, enc_terms, dn)

    over_columns(part_of_enc_terms_den)
    enc_x = send(xt, rxd.at[0], x_dev)

    def self_back(j, hooks):
        arrived(4, j)
        norm_back(j, 4, gains[0], n1, r1, 0, 9, 12)
        if j == 1:
            sent(gsend[1])
            grad_into(send_of[3], [(ct, head_cols(ao, nc))])
            launch(gsend[4])
            grad_into(own_of[3], [(ct, head_cols(ao, c))])
        heads_back(j, wb, 0, qs, ks, vs, ao, lse1, True, hooks)

    self_back(0, ({2: part(grad_core, 3)}, {2: part(grad_y, 1)}))
    sent(enc_x)
    self_back(1, ({2: part(grad_y, 2), 6: part(grad_core, 4)}, {4: part(grad_z, 0, ge_out)}))
    sent(swap2)
    swap1 = swap_kv(1)
    l_x2a.wait()
    l_x2b.wait()
    grad_into(send_of[3], [(x1r, head_cols(dq, nc))], 256)
    launch(gsend[5])
    grad_into(own_of[3], [(x1r, head_cols(dq, c))], 256)
    for j in range(2):
        for q in range(2):
            sum_rows(3, dq[j, :, q * 256 : q * 256 + 256], x * 512 + q * 256)
    swap1.wait_recv()
    join_kv(1)
    grad_into(send_of[3], [(x1r, head_cols(krecv.at[1, i], nc)) for i in range(2)], 512)
    launch(gsend[6])
    launch(gsend[7])
    grad_core(5)
    grad_y(3)
    in_terms = [(dq, wa, 0), (krecv.at[1, 0], wa, 256), (krecv.at[1, 1], wa, 512)]
    def part_of_in_terms_xt(dn, cols):
        xt[:, cols] = input_part(nx, in_terms, dn).astype(BF)

    over_columns(part_of_in_terms_xt)
    hid_x = send(xt, rxd.at[1], x_dev)
    grad_into(own_of[3], [(x1r, head_cols(krecv.at[1, i], c)) for i in range(2)], 512)
    grad_core(6)
    grad_core(7)
    for j in range(2):
        for q in range(2):
            sum_rows(4, krecv[1, 1, j, :, q * 256 : q * 256 + 256], x * 512 + q * 256)
    s1 = send(sm, smr.at[0], c_dev)
    grad_y(4)
    def part_of_in_terms_res(dn, cols):
        res[x, :, cols] += input_part(x, in_terms, dn)

    over_columns(part_of_in_terms_res)
    s1.wait_recv()
    sent(s1)
    sm[...] += smr[0]
    s2 = send(sm, smr.at[1], x_dev)
    sent(hid_x)
    enc_x.wait_recv()
    den[...] += rxd[0].astype(F32)
    o1 = local(den, enc_out)
    grad_y(5)
    s2.wait_recv()
    sent(s2)
    sm[...] += smr[1]
    s3 = send(sm, smr.at[2], y_dev)
    grad_z(1, gs_out)
    hid_x.wait_recv()
    res[x] += rxd[1].astype(F32)
    o2 = local(res.at[x], hid_out)
    grad_y(6)
    s3.wait_recv()
    sent(s3)
    sm[...] += smr[2]
    smz[z] = sm[...]
    s4 = [send(sm, smz.at[z], z_dev(k)) for k in range(1, nz)]
    grad_y(7)
    grad_z(2, gc_out)
    grad_z(3, gc_out)
    grad_z(4, ga_out)
    grad_z(5, ga_out)
    for cp in s4:
        cp.wait_recv()
        sent(cp)
    acc = smz[0]
    for k in range(1, nz):
        acc = acc + smz[k]
    for row in range(3):
        gain_out[row] = acc[row : row + 1, :]
    for row in range(9):
        bias_out[row] = acc[row + 3 : row + 4, :]
    selfb_out[...] = acc[12:13, :]
    for row in range(4):
        expb_out[:, row * 1024 : row * 1024 + 1024] = acc[row + 13 : row + 14, :]
    grad_z(6, ga_out)
    grad_z(7, ga_out)
    for cp in [o1, o2] + list(out_copies.values()):
        cp.wait()
    for cp in list(pending):
        sent(cp)


def run_layer(nz, sh, prefix, hid, enc, cot, shards, gains, biases, selfb, expb):
    any_spec = pl.BlockSpec(memory_space=pl.ANY)
    vmem = pl.BlockSpec(memory_space=pltpu.VMEM)
    rows = hid.shape[0]
    shape = jax.ShapeDtypeStruct
    outs = [
        shape((rows, 1024), BF),
        shape((rows, 1024), F32),
        shape((rows, 1024), F32),
        shape((sh, 1024), F32),
        shape((sh, 1024), F32),
        shape((sh, 1024), F32),
        shape((sh, 1024), F32),
        shape((3, 1, 1024), F32),
        shape((9, 1, 1024), F32),
        shape((1, 1024), F32),
        shape((1, 4096), F32),
        shape((2, rows, 1024), BF),
        shape((2, rows, 1024), BF),
        shape((4, nz, 2, sh, 1024), BF),
        shape((4, nz, sh, 1024), BF),
        shape((4, nz, sh, 1024), BF),
    ]

    def weight(n):
        return pltpu.VMEM((2, nz, 2, sh, n), BF)

    def acts(n, kind=BF):
        return pltpu.VMEM((2, rows, n), kind)

    def keys(kind=BF):
        return pltpu.VMEM((4, rows, 512), kind)

    scratch = [
        weight(768),
        weight(768),
        weight(512),
        weight(1024),
        weight(1024),
        acts(1024),
        acts(1024),
        acts(1024),
        acts(512),
        keys(),
        keys(),
        acts(512),
        acts(512),
        keys(),
        keys(),
        acts(512),
        pltpu.VMEM((2, 2, rows, 1024), BF),
        pltpu.VMEM((2, 2, rows, 1024), BF),
        acts(1024),
        acts(1024),
        acts(128, F32),
        acts(128, F32),
        acts(128, F32),
        acts(128, F32),
        acts(1024, F32),
        acts(1024),
        pltpu.VMEM((2, 2, rows, 1024), BF),
        acts(1024),
        acts(512),
        pltpu.VMEM((rows, 512), BF),
        keys(F32),
        keys(F32),
        pltpu.VMEM((2, 2, rows, 512), BF),
        pltpu.VMEM((2, 2, 2, rows, 512), BF),
        pltpu.VMEM((2, 1024, 1024), BF),
        pltpu.VMEM((2, nz, 2, sh, 1024), BF),
        pltpu.VMEM((nz, 2, sh, 1024), BF),
        pltpu.VMEM((rows, 1024), BF),
        pltpu.VMEM((1024, 256), BF),
        pltpu.VMEM((1024, 256), BF),
        pltpu.VMEM((rows, 1024), F32),
        pltpu.VMEM((2, sh, 1024), F32),
        pltpu.VMEM((SMALL_ROWS, 1024), F32),
        pltpu.VMEM((3, SMALL_ROWS, 1024), F32),
        pltpu.VMEM((nz, SMALL_ROWS, 1024), F32),
        pltpu.SemaphoreType.DMA((280 + 64 * nz,)),
    ]
    return pl.pallas_call(
        functools.partial(layer_kernel, nz, sh),
        out_shape=outs,
        in_specs=[pl.BlockSpec(memory_space=pltpu.SMEM)] + [any_spec] * 13 + [vmem] * 4,
        out_specs=[any_spec] * 7 + [vmem] * 4 + [any_spec] * (len(outs) - 11),
        scratch_shapes=scratch,
        compiler_params=pltpu.CompilerParams(
            collective_id=0, has_side_effects=True, vmem_limit_bytes=67043328
        ),
    )(prefix, hid, enc, cot, *shards, gains, biases, selfb, expb)


def per_device(
    hidden,
    encoder,
    prefix,
    query_self,
    key_self,
    value_self,
    output_self,
    cross_query_matrix,
    key_cross,
    value_cross,
    output_cross,
    expand,
    shrink,
    norm_gains,
    biases,
    self_out_bias,
    expand_bias,
    cotangent,
):
    sh = query_self.shape[1]
    nz = 1024 // sh // 2
    shards = (
        query_self[0],
        key_self[0],
        value_self[0],
        output_self[0].T,
        key_cross[0],
        value_cross[0],
        cross_query_matrix[0],
        output_cross[0].T,
        expand[0],
        shrink[0].T,
    )
    outs = run_layer(
        nz,
        sh,
        prefix,
        hidden[0],
        encoder[0],
        cotangent[0],
        shards,
        jnp.swapaxes(norm_gains, 0, 1),
        jnp.swapaxes(biases, 0, 1),
        self_out_bias,
        expand_bias,
    )
    block, grad_hid, grad_enc, ge, gs, gc, ga, gain, bias, selfb, expb = outs[:11]

    def part(g, i):
        return g[:, i * 256 : i * 256 + 256]

    return (
        block[None],
        grad_hid[None],
        grad_enc[None],
        part(ga, 1)[None],
        part(ga, 2)[None],
        part(ga, 3)[None],
        part(ga, 0).T[None],
        part(gc, 1)[None],
        part(gc, 2)[None],
        part(gc, 3)[None],
        part(gc, 0).T[None],
        ge[None],
        gs.T[None],
        jnp.swapaxes(gain, 0, 1),
        jnp.swapaxes(bias, 0, 1),
        selfb,
        expb,
    )


def solution(mesh):
    in_specs = (
        P("dp", "tensor", None),
        P("dp", "tensor", None),
        P("dp"),
        P(None, "dp", "tensor"),
        P(None, "dp", "tensor"),
        P(None, "dp", "tensor"),
        P(None, "tensor", "dp"),
        P(None, "dp", "tensor"),
        P(None, "dp", "tensor"),
        P(None, "dp", "tensor"),
        P(None, "tensor", "dp"),
        P(None, "dp", "tensor"),
        P(None, "tensor", "dp"),
        P(),
        P(),
        P(),
        P(),
        P("dp", "tensor", None),
    )
    out_specs = (
        P("dp", "tensor", None),
        P("dp", "tensor", None),
        P("dp", "tensor", None),
        P(None, "dp", "tensor"),
        P(None, "dp", "tensor"),
        P(None, "dp", "tensor"),
        P(None, "tensor", "dp"),
        P(None, "dp", "tensor"),
        P(None, "dp", "tensor"),
        P(None, "dp", "tensor"),
        P(None, "tensor", "dp"),
        P(None, "dp", "tensor"),
        P(None, "tensor", "dp"),
        P(),
        P(),
        P(),
        P(),
    )
    return jax.shard_map(
        per_device, mesh=mesh, in_specs=in_specs, out_specs=out_specs, check_vma=False
    )
```
